32 devices in a mesh: rep: 2 (over z, core), dp: 16 (over x, y).
Axes of the slice: x: 4, y: 4, z: 1, core: 2. Of those that a mesh axis runs over, the one named last changes fastest.
The devices are a block of a 4x4x8 slice.
Arguments:
- x: bfloat16 [32, 2048, 640], P(('rep', 'dp')), parts along dimension 0
- dy: bfloat16 [32, 2048, 640], P(('rep', 'dp')), parts along dimension 0
- w_gate: bfloat16 [2, 640, 2048], replicated
- w_up: bfloat16 [2, 640, 2048], replicated
- w_down: bfloat16 [2, 2048, 640], replicated
- m_w_gate: float32 [2, 640, 2048], P(None, 'dp')
- m_w_up: float32 [2, 640, 2048], P(None, 'dp')
- m_w_down: float32 [2, 2048, 640], P(None, 'dp')
- v_w_gate: float32 [2, 640, 2048], P(None, 'dp')
- v_w_up: float32 [2, 640, 2048], P(None, 'dp')
- v_w_down: float32 [2, 2048, 640], P(None, 'dp')
Outputs:
- output 1: bfloat16 [4, 640, 2048], P('rep'), parts along dimension 0
- output 2: bfloat16 [4, 640, 2048], P('rep'), parts along dimension 0
- output 3: bfloat16 [4, 2048, 640], P('rep'), parts along dimension 0
- output 4: float32 [4, 640, 2048], P('rep', 'dp'), parts along dimension 0
- output 5: float32 [4, 640, 2048], P('rep', 'dp'), parts along dimension 0
- output 6: float32 [4, 2048, 640], P('rep', 'dp'), parts along dimension 0
- output 7: float32 [4, 640, 2048], P('rep', 'dp'), parts along dimension 0
- output 8: float32 [4, 640, 2048], P('rep', 'dp'), parts along dimension 0
- output 9: float32 [4, 2048, 640], P('rep', 'dp'), parts along dimension 0
There are 2 independent parts. The reference program is written for one: setup_inputs(seed, part) draws one part's arguments, and reference() takes and returns one part's arrays. A program takes and returns all parts, laid end to end along the dimension named above; an argument that names none is the same for every part.
All inputs are finite; a program needn't handle non-finite values.
Results may differ from the reference program's by a relative error of at most 0.022.
Values are sent between devices in bfloat16 or wider.
A program may use at most 768 MiB of HBM per device.

```python
import jax
import jax.numpy as jnp
from jax import lax

SEQUENCES = 16
TOKENS = 2048
D = 640
FF = 2048
LAYERS = 2
NAMES = ("w_gate", "w_up", "w_down")
SHAPES = {"w_gate": (LAYERS, D, FF), "w_up": (LAYERS, D, FF), "w_down": (LAYERS, FF, D)}


def bump(key, n, height):
    away = (jnp.arange(n, dtype=jnp.int32) - jax.random.randint(key, (), 0, n, jnp.int32)) % n
    return jnp.where(away < n // 8, height, 1.0)


def together(key, own, strength):
    shared = jax.random.normal(key, own.shape[1:], jnp.float32)
    return (own + strength * shared) * lax.rsqrt(1 + strength * strength)


def setup_inputs(seed: int = 0, part: int = 0) -> dict:
    kx, kdy, ka, kb, kz, kf, kh, kl, *keys = jax.random.split(jax.random.key(seed), 8 + 3 * len(NAMES))
    kx, kdy, ka, kb = (jax.random.fold_in(k, part) for k in (kx, kdy, ka, kb))
    kw, km, kv = (keys[i::3] for i in range(3))
    shape = (SEQUENCES, TOKENS, D)
    much_x, much_dy = jax.random.uniform(kz, (2,), jnp.float32, 0.0, 1.0)
    loud = 2.0 ** jax.random.uniform(jax.random.fold_in(kz, 1), (), jnp.float32, -1.0, 2.0)
    layers = 2.0 ** jax.random.uniform(kl, (LAYERS, 1, 1), jnp.float32, -1.0, 1.0)
    x = together(ka, jax.random.normal(kx, shape, jnp.float32), much_x) * bump(kf, D, 4.0)
    dy = together(kb, jax.random.normal(kdy, shape, jnp.float32), much_dy)
    drawn = {"x": x.astype(jnp.bfloat16), "dy": (loud * dy * (SEQUENCES * TOKENS) ** -0.5).astype(jnp.bfloat16)}
    for key, name in zip(kw, NAMES, strict=True):
        w = jax.random.normal(key, SHAPES[name], jnp.float32) * SHAPES[name][1] ** -0.5
        drawn[name] = (w * {"w_gate": 1.0, "w_up": bump(kh, FF, 4.0), "w_down": layers}[name]).astype(jnp.bfloat16)
    for key, name in zip(km, NAMES, strict=True):
        drawn[f"m_{name}"] = 0.1 * jax.random.normal(key, SHAPES[name], jnp.float32)
    for key, name in zip(kv, NAMES, strict=True):
        drawn[f"v_{name}"] = jax.random.uniform(key, SHAPES[name], jnp.float32, 0.005, 0.015)
    return drawn


def matmul(a, w):
    return jnp.dot(a, w, preferred_element_type=jnp.float32).astype(jnp.bfloat16)


def normed(h):
    wide = h.astype(jnp.float32)
    scale = lax.rsqrt(jnp.mean(wide**2, -1, keepdims=True) + 1e-6)
    return (wide * scale).astype(jnp.bfloat16)


def layer(h, w):
    a = normed(h)
    gate = jnp.dot(a, w["w_gate"], preferred_element_type=jnp.float32)
    up = jnp.dot(a, w["w_up"], preferred_element_type=jnp.float32)
    return h + matmul((jax.nn.silu(gate) * up).astype(jnp.bfloat16), w["w_down"])


def adamw(w, m, v, g):
    m = 0.9 * m + 0.1 * g
    v = 0.95 * v + 0.05 * g * g
    step = m * lax.rsqrt(v + 1e-8) + 0.1 * w
    return (w - 0.02 * step).astype(jnp.bfloat16), m, v


def clipped(gradients, sum_of_squares, count):
    factor = jnp.minimum(1.0, 0.5 * lax.rsqrt(sum_of_squares / count + 1e-30))
    return [g * factor for g in gradients]


def stack(weights, h):
    return lax.scan(lambda h, w: (layer(h, w), None), h, weights)[0]


def reference(x, dy, w_gate, w_up, w_down, m_w_gate, m_w_up, m_w_down, v_w_gate, v_w_up, v_w_down):
    weights = dict(zip(NAMES, (w_gate, w_up, w_down), strict=True))

    def take(so_far, sequence):
        h, by_y = sequence
        _, back = jax.vjp(lambda w: stack(w, h), weights)
        return jax.tree.map(lambda total, term: total + term.astype(jnp.float32), so_far, back(by_y)[0]), None

    none_yet = {name: jnp.zeros(w.shape, jnp.float32) for name, w in weights.items()}
    by_weights, _ = lax.scan(take, none_yet, (x, dy))
    gradients = [by_weights[name].astype(jnp.bfloat16).astype(jnp.float32) for name in NAMES]
    gradients = clipped(gradients, sum(jnp.sum(g * g) for g in gradients), sum(g.size for g in gradients))
    new = [
        adamw(w.astype(jnp.float32), m, v, g)
        for w, m, v, g in zip((w_gate, w_up, w_down), (m_w_gate, m_w_up, m_w_down), (v_w_gate, v_w_up, v_w_down), gradients, strict=True)
    ]
    return tuple(one[which] for which in range(3) for one in new)
```

```python
import functools
import math

import jax
import jax.numpy as jnp
from jax import lax
from jax.experimental import pallas as pl
from jax.experimental.pallas import tpu as pltpu
from jax.sharding import PartitionSpec as P

MESH = pl.DeviceIdType.MESH
F32, BF16 = jnp.float32, jnp.bfloat16
QUARTERS = 4
PIECES = 2


def matmul(a, w):
    return jnp.dot(a, w, preferred_element_type=F32).astype(BF16)


def normed(h):
    wide = h.astype(F32)
    scale = lax.rsqrt(jnp.mean(wide**2, -1, keepdims=True) + 1e-6)
    return (wide * scale).astype(BF16)


def layer(h, gate_w, up_w, down_w):
    a = normed(h)
    gate = jnp.dot(a, gate_w, preferred_element_type=F32)
    up = jnp.dot(a, up_w, preferred_element_type=F32)
    return h + matmul((jax.nn.silu(gate) * up).astype(BF16), down_w)


def adamw(w, m, v, g):
    m = 0.9 * m + 0.1 * g
    v = 0.95 * v + 0.05 * g * g
    step = m * lax.rsqrt(v + 1e-8) + 0.1 * w
    return (w - 0.02 * step).astype(BF16), m, v


def sync_kernel(side, layers, count, *refs):
    n = side * side
    grads, rest = refs[: 3 * layers], refs[3 * layers :]
    w_gate, w_up, w_down, m_gate, m_up, m_down, v_gate, v_up, v_down = rest[:9]
    new_gu, new_d, nm_gate, nm_up, nm_down, nv_gate, nv_up, nv_down = rest[9:17]
    (loc_gu, loc_d, in1_gu, in1_d, in2_gu, in2_d, sum_gu, sum_d, own_gu, own_d, norms, tile) = rest[17:29]
    load_sem, send_gu, recv_gu, send_d, recv_d, norm_send, norm_recv, keep_sem = rest[29:]
    me = lax.axis_index("dp")
    row, col = lax.div(me, side), lax.rem(me, side)
    cols = loc_gu.shape[-1]
    width = cols // PIECES // QUARTERS

    loads = []
    for l in range(layers):
        g, u, d = grads[3 * l : 3 * l + 3]
        loads.append([
            pltpu.make_async_copy(src, dst, load_sem.at[l, k])
            for k, (src, dst) in enumerate(((g, loc_gu.at[0, l]), (u, loc_gu.at[1, l]), (d, loc_d.at[l])))
        ])
    for some in loads:
        for one in some:
            one.start()

    barrier = pltpu.get_barrier_semaphore()

    def greet(k, _):
        pl.semaphore_signal(barrier, inc=1, device_id={"dp": lax.rem(me + k, n)}, device_id_type=MESH)
        return _

    lax.fori_loop(1, n, greet, 0)
    pl.semaphore_wait(barrier, n - 1)

    def place(q):
        return (row, col) if q < 2 else (col, row)

    def device(q, u, v):
        u, v = lax.rem(u + 2 * side, side), lax.rem(v + 2 * side, side)
        return {"dp": u * side + v if q < 2 else v * side + u}

    def sign(q):
        return 1 if q % 2 == 0 else -1

    def wrap(k):
        return lax.rem(k + 2 * side, side)

    def lanes(h, q):
        return pl.ds(pl.multiple_of((h * QUARTERS + q) * width, 128), width)

    def sems(l, h, q, s):
        if h is None:
            return send_d.at[l, q, s], recv_d.at[l, q, s]
        return send_gu.at[l, h, q, s], recv_gu.at[l, h, q, s]

    def local_unit(l, h, q, u):
        if h is None:
            return loc_d.at[l, u, :, q] if q < 2 else loc_d.at[l, :, u, q]
        at = lanes(h, q)
        return loc_gu.at[:, l, u, :, :, at] if q < 2 else loc_gu.at[:, l, :, u, :, at]

    def local_value(l, h, q, u, v):
        a, b = (u, v) if q < 2 else (v, u)
        if h is None:
            return loc_d[l, a, b, q]
        return loc_gu[:, l, a, b, :, lanes(h, q)]

    def first(l, h, q, s):
        mu, mv = place(q)
        g = sign(q)
        dst = in1_d.at[l, q, s] if h is None else in1_gu.at[l, h, q, s]
        if s == 0:
            src = local_unit(l, h, q, wrap(mu - g))
        else:
            src = in1_d.at[l, q, s - 1] if h is None else in1_gu.at[l, h, q, s - 1]
        a, b = sems(l, h, q, s)
        return pltpu.make_async_remote_copy(src, dst, a, b, device_id=device(q, mu + g, mv), device_id_type=MESH)

    def second(l, h, q, s):
        mu, mv = place(q)
        g = sign(q)
        dst = in2_d.at[l, q, s] if h is None else in2_gu.at[l, h, q, s]
        if s == 0:
            v = wrap(mv - g)
            src = in1_d.at[l, q, 2, v] if h is None else in1_gu.at[l, h, q, 2, :, v]
        else:
            src = in2_d.at[l, q, s - 1] if h is None else in2_gu.at[l, h, q, s - 1]
        a, b = sems(l, h, q, 3 + s)
        return pltpu.make_async_remote_copy(src, dst, a, b, device_id=device(q, mu, mv + g), device_id_type=MESH)

    def add_first(l, h, q, s):
        u = wrap(place(q)[0] - sign(q) * (s + 2))

        def one(v, _):
            mine = local_value(l, h, q, u, v).astype(F32)
            if h is None:
                in1_d[l, q, s, v] = (in1_d[l, q, s, v].astype(F32) + mine).astype(BF16)
            else:
                in1_gu[l, h, q, s, :, v] = (in1_gu[l, h, q, s, :, v].astype(F32) + mine).astype(BF16)
            return _

        lax.fori_loop(0, side, one, 0)

    def add_second(l, h, q, s):
        v = wrap(place(q)[1] - sign(q) * (s + 2))
        if h is None:
            total = (in2_d[l, q, s].astype(F32) + in1_d[l, q, 2, v].astype(F32)).astype(BF16)
        else:
            total = (in2_gu[l, h, q, s].astype(F32) + in1_gu[l, h, q, 2, :, v].astype(F32)).astype(BF16)
        if s < side - 2:
            if h is None:
                in2_d[l, q, s] = total
            else:
                in2_gu[l, h, q, s] = total
            return
        total = total.astype(F32)
        if h is None:
            sum_d[l, q] = total
        else:
            sum_gu[:, l, :, lanes(h, q)] = total
        square = total * total
        square = square.reshape(-1, 8, square.shape[-1]).sum(0)
        tile[...] += sum(square[:, k : k + 128] for k in range(0, square.shape[-1], 128))

    def jobs(f):
        for l in reversed(range(layers)):
            lax.fori_loop(0, PIECES, lambda h, _: (f(l, h), _)[1], 0)
            f(l, None)

    steps = side - 1
    for l in reversed(range(layers)):
        for one in loads[l]:
            one.wait()
    tile[...] = jnp.zeros_like(tile)

    def begin(l, h):
        for q in range(QUARTERS):
            first(l, h, q, 0).start()

    jobs(begin)
    for s in range(steps):
        def advance(l, h, s=s):
            for q in range(QUARTERS):
                first(l, h, q, s).wait()
                add_first(l, h, q, s)
                (first(l, h, q, s + 1) if s + 1 < steps else second(l, h, q, 0)).start()

        jobs(advance)
    for s in range(steps):
        def advance(l, h, s=s):
            for q in range(QUARTERS):
                second(l, h, q, s).wait()
                add_second(l, h, q, s)
                if s + 1 < steps:
                    second(l, h, q, s + 1).start()

        jobs(advance)

    norms[me] = tile[...]

    def share(k):
        return pltpu.make_async_remote_copy(
            tile, norms.at[me], norm_send.at[k], norm_recv.at[k], device_id={"dp": lax.rem(me + k, n)}, device_id_type=MESH)

    lax.fori_loop(1, n, lambda k, _: (share(k).start(), _)[1], 0)
    lax.fori_loop(1, n, lambda k, _: (share(k).wait(), _)[1], 0)
    total = jnp.sum(jnp.sum(norms[...], axis=0))
    factor = jnp.minimum(1.0, 0.5 * lax.rsqrt(jnp.full((1, 128), total, F32) / count + 1e-30))

    def gather(l, h, q, s):
        mu, mv = place(q)
        g = sign(q)
        if s < steps:
            v = wrap(mv - g * s)
            a, b = (mu, v) if q < 2 else (v, mu)
            dst = new_d.at[l, a, b, q] if h is None else new_gu.at[:, l, a, b, :, lanes(h, q)]
            src = dst
            if s == 0:
                src = own_d.at[l, q] if h is None else own_gu.at[:, l, :, lanes(h, q)]
            to = device(q, mu, mv + g)
        else:
            u = wrap(mu - g * (s - steps))
            if h is None:
                dst = new_d.at[l, u, :, q] if q < 2 else new_d.at[l, :, u, q]
            else:
                at = lanes(h, q)
                dst = new_gu.at[:, l, u, :, :, at] if q < 2 else new_gu.at[:, l, :, u, :, at]
            src = dst
            to = device(q, mu + g, mv)
        a, b = sems(l, h, q, s)
        return pltpu.make_async_remote_copy(src, dst, a, b, device_id=to, device_id_type=MESH)

    def keep(l, d):
        if d:
            return pltpu.make_async_copy(own_d.at[l], new_d.at[l, row, col], keep_sem.at[l, 1])
        return pltpu.make_async_copy(own_gu.at[:, l], new_gu.at[:, l, row, col], keep_sem.at[l, 0])

    for l in reversed(range(layers)):
        for h in range(PIECES):
            for q in range(QUARTERS):
                at = pl.ds((h * QUARTERS + q) * width, width)
                by = jnp.tile(factor, (1, width // 128))
                for k, (w, m, v, nm, nv) in enumerate(((w_gate, m_gate, v_gate, nm_gate, nv_gate), (w_up, m_up, v_up, nm_up, nv_up))):
                    new, nm[l, :, at], nv[l, :, at] = adamw(
                        w[l, :, at].astype(F32), m[l, :, at], v[l, :, at], sum_gu[k, l, :, at] * by)
                    own_gu[k, l, :, at] = new
                gather(l, h, q, 0).start()
        keep(l, False).start()
        for q in range(QUARTERS):
            rows = m_down.shape[1] // QUARTERS
            at = pl.ds(q * rows, rows)
            by = jnp.tile(factor, (1, m_down.shape[2] // 128))
            new, nm_down[l, at], nv_down[l, at] = adamw(
                w_down[l, at].astype(F32), m_down[l, at], v_down[l, at], sum_d[l, q] * by)
            own_d[l, q] = new
            gather(l, None, q, 0).start()
        keep(l, True).start()
    for l in reversed(range(layers)):
        keep(l, False).wait()
        keep(l, True).wait()
    for s in range(2 * steps):
        def advance(l, h, s=s):
            for q in range(QUARTERS):
                gather(l, h, q, s).wait()
                if s + 1 < 2 * steps:
                    gather(l, h, q, s + 1).start()

        jobs(advance)


def sync(side, grads, own, m, v):
    layers, rows, cols = m[0].shape
    deep, narrow = m[2].shape[1:]
    quarter = deep // QUARTERS
    width = cols // PIECES // QUARTERS
    n = side * side
    steps = side - 1
    count = layers * n * (2 * rows * cols + deep * narrow)
    shaped = []
    for l in range(layers):
        g, u, d = (grads[k][l] for k in range(3))
        shaped += [g.reshape(side, side, rows, cols), u.reshape(side, side, rows, cols), d.reshape(side, side, QUARTERS, quarter, narrow)]
    vmem, hbm = pl.BlockSpec(memory_space=pltpu.VMEM), pl.BlockSpec(memory_space=pl.ANY)
    outs = pl.pallas_call(
        functools.partial(sync_kernel, side, layers, count),
        out_shape=[
            jax.ShapeDtypeStruct((2, layers, side, side, rows, cols), BF16),
            jax.ShapeDtypeStruct((layers, side, side, QUARTERS, quarter, narrow), BF16),
            *(jax.ShapeDtypeStruct(t.shape, F32) for t in (*m, *v)),
        ],
        in_specs=[hbm] * (3 * layers) + [vmem] * 9,
        out_specs=[hbm] * 2 + [vmem] * 6,
        scratch_shapes=[
            pltpu.VMEM((2, layers, side, side, rows, cols), BF16),
            pltpu.VMEM((layers, side, side, QUARTERS, quarter, narrow), BF16),
            pltpu.VMEM((layers, PIECES, QUARTERS, steps, 2, side, rows, width), BF16),
            pltpu.VMEM((layers, QUARTERS, steps, side, quarter, narrow), BF16),
            pltpu.VMEM((layers, PIECES, QUARTERS, steps, 2, rows, width), BF16),
            pltpu.VMEM((layers, QUARTERS, steps, quarter, narrow), BF16),
            pltpu.VMEM((2, layers, rows, cols), F32),
            pltpu.VMEM((layers, QUARTERS, quarter, narrow), F32),
            pltpu.VMEM((2, layers, rows, cols), BF16),
            pltpu.VMEM((layers, QUARTERS, quarter, narrow), BF16),
            pltpu.VMEM((n, 8, 128), F32),
            pltpu.VMEM((8, 128), F32),
            pltpu.SemaphoreType.DMA((layers, 3)),
            pltpu.SemaphoreType.DMA((layers, PIECES, QUARTERS, 2 * steps)),
            pltpu.SemaphoreType.DMA((layers, PIECES, QUARTERS, 2 * steps)),
            pltpu.SemaphoreType.DMA((layers, QUARTERS, 2 * steps)),
            pltpu.SemaphoreType.DMA((layers, QUARTERS, 2 * steps)),
            pltpu.SemaphoreType.DMA((n,)),
            pltpu.SemaphoreType.DMA((n,)),
            pltpu.SemaphoreType.DMA((layers, 2)),
        ],
        compiler_params=pltpu.CompilerParams(collective_id=0, has_side_effects=True, vmem_limit_bytes=60 * 2**20),
    )(*shaped, *own, *m, *v)
    gu = outs[0].reshape(2, layers, n * rows, cols)
    return (gu[0], gu[1], outs[1].reshape(layers, n * deep, narrow), *outs[2:])


def solution(mesh):
    side = math.isqrt(mesh.shape["dp"])

    def step(x, dy, *arrays):
        weights, m, v = (arrays[i : i + 3] for i in (0, 3, 6))
        layers = weights[0].shape[0]

        def stack(w):
            h = x
            for one in w:
                h = layer(h, *one)
            return h

        _, back = jax.vjp(stack, [tuple(w[l] for w in weights) for l in range(layers)])
        by = back(dy)[0]
        grads = [[by[l][k] for l in range(layers)] for k in range(3)]
        me = lax.axis_index("dp")
        own = [lax.dynamic_slice_in_dim(w, me * t.shape[1], t.shape[1], 1) for w, t in zip(weights, m, strict=True)]
        return sync(side, grads, own, m, v)

    whole, block = P(None, None, None), P(None, "dp", None)
    return jax.shard_map(
        step,
        mesh=mesh,
        in_specs=(P(("rep", "dp"), None, None),) * 2 + (whole,) * 3 + (block,) * 6,
        out_specs=(P("rep", None, None),) * 3 + (P("rep", "dp", None),) * 6,
        check_vma=False,
    )
```

```python
import functools
import math

import jax
import jax.numpy as jnp
from jax import lax
from jax.experimental import pallas as pl
from jax.experimental.pallas import tpu as pltpu
from jax.sharding import PartitionSpec as P

MESH = pl.DeviceIdType.MESH
F32, BF16 = jnp.float32, jnp.bfloat16
QUARTERS = 4
PIECES = 2


NT = (((1,), (1,)), ((), ()))

def dot(a, b): return jnp.dot(a, b, preferred_element_type=F32)
def dot_nt(a, b): return lax.dot_general(a, b, NT, preferred_element_type=F32)

def normed(h):
    wide = h.astype(F32)
    scale = lax.rsqrt(jnp.mean(wide**2, -1, keepdims=True) + 1e-6)
    return (wide * scale).astype(BF16)

def forward_kernel(x, dy, wg, wu, wd, a0, a0t, h1, a1, a1t, dyt):
    a = normed(x[...])
    a0[...] = a
    a0t[...] = a.T
    dyt[...] = dy[...].T
    gate = dot(a, wg[...])
    up = dot(a, wu[...])
    p = (jax.nn.silu(gate) * up).astype(BF16)
    h = x[...] + dot(p, wd[...]).astype(BF16)
    h1[...] = h
    b = normed(h)
    a1[...] = b
    a1t[...] = b.T

def forward(x, dy, wg, wu, wd, T=256):
    n, d = x.shape
    f = wg.shape[1]
    tile = pl.BlockSpec((T, d), lambda i: (i, 0))
    tilet = pl.BlockSpec((d, T), lambda i: (0, i))
    const = lambda s: pl.BlockSpec(s, lambda i: (0, 0), pipeline_mode=pl.Buffered(1))
    S = jax.ShapeDtypeStruct
    return pl.pallas_call(
        forward_kernel, grid=(n // T,),
        in_specs=[tile, tile, const((d, f)), const((d, f)), const((f, d))],
        out_specs=[tile, tilet, tile, tile, tilet, tilet],
        out_shape=[S((n, d), BF16), S((d, n), BF16), S((n, d), BF16), S((n, d), BF16), S((d, n), BF16), S((d, n), BF16)],
        compiler_params=pltpu.CompilerParams(vmem_limit_bytes=60 * 2**20),
        name="fwd",
    )(x, dy, wg, wu, wd)

def tile_step(a, dy, wg, wu, wd):
    gate = dot(a, wg)
    up = dot(a, wu)
    dp = dot_nt(dy, wd).astype(BF16).astype(F32)
    s = jax.nn.sigmoid(gate)
    act = gate * s
    p = (act * up).astype(BF16)
    du = (dp * act).astype(BF16)
    dg = (dp * up * (s + act * (1.0 - s))).astype(BF16)
    return p, dg, du

def norm_back(h, da, dy):
    wide = h.astype(F32)
    d = h.shape[-1]
    scale = lax.rsqrt(jnp.mean(wide**2, -1, keepdims=True) + 1e-6)
    along = jnp.sum(da * wide, -1, keepdims=True)
    back = da * scale - wide * (along * (scale * scale * scale) * (1.0 / d))
    return (dy.astype(F32) + back.astype(BF16).astype(F32)).astype(BF16)

def backward_kernel(T, F, inner, *refs):
    if inner:
        h, a, at, dy, dyt, wg, wu, wd, og, ou, od, dh, dht, ps, gs, us, das = refs
    else:
        a, at, dy, dyt, wg, wu, wd, og, ou, od, ps, gs, us = refs
    n, d = a.shape
    f = wg.shape[1]
    if inner:
        das[...] = jnp.zeros_like(das)
    def chunk(c, _):
        cs = pl.ds(pl.multiple_of(c * F, F), F)
        for t in range(n // T):
            ts = pl.ds(t * T, T)
            p, dg, du = tile_step(a[ts], dy[ts], wg[:, cs], wu[:, cs], wd[cs])
            ps[ts] = p
            gs[ts] = dg
            us[ts] = du
            if inner:
                das[ts] += dot_nt(dg, wg[:, cs]) + dot_nt(du, wu[:, cs])
        og[:, cs] = dot(at[...], gs[...]).astype(BF16)
        ou[:, cs] = dot(at[...], us[...]).astype(BF16)
        by_down = dot(dyt[...], ps[...]).astype(BF16)
        wide = od.shape[-1]
        for k in range(F // wide):
            od[c * (F // wide) + k] = by_down[:, k * wide : (k + 1) * wide]
        return _
    lax.fori_loop(0, f // F, chunk, 0)
    if inner:
        def fin(t, _):
            ts = pl.ds(pl.multiple_of(t * 256, 256), 256)
            r = norm_back(h[ts], das[ts].astype(BF16).astype(F32), dy[ts])
            dh[ts] = r
            dht[:, ts] = r.T
            return _
        lax.fori_loop(0, n // 256, fin, 0)

def backward(inner, *args, wide, T=512, F=512):
    a = args[1] if inner else args[0]
    n, d = a.shape
    f = args[-1].shape[0]
    S = jax.ShapeDtypeStruct
    out = [S((d, f), BF16)] * 2 + [S((f // wide, d, wide), BF16)] + ([S((n, d), BF16), S((d, n), BF16)] if inner else [])
    scr = [pltpu.VMEM((n, F), BF16)] * 3 + ([pltpu.VMEM((n, d), F32)] if inner else [])
    v = pl.BlockSpec(memory_space=pltpu.VMEM)
    return pl.pallas_call(
        functools.partial(backward_kernel, T, F, inner),
        in_specs=[v] * len(args), out_specs=[v] * len(out), out_shape=out, scratch_shapes=scr,
        compiler_params=pltpu.CompilerParams(vmem_limit_bytes=63 * 2**20), name="bwd1" if inner else "bwd0",
    )(*args)

def adamw(w, m, v, g):
    m = 0.9 * m + 0.1 * g
    v = 0.95 * v + 0.05 * g * g
    step = m * lax.rsqrt(v + 1e-8) + 0.1 * w
    return (w - 0.02 * step).astype(BF16), m, v


def sync_kernel(side, layers, count, *refs):
    n = side * side
    grads, rest = refs[: 3 * layers], refs[3 * layers :]
    w_gate, w_up, w_down, m_gate, m_up, m_down, v_gate, v_up, v_down = rest[:9]
    new_gu, new_d, nm_gate, nm_up, nm_down, nv_gate, nv_up, nv_down = rest[9:17]
    (loc_gu, loc_d, in1_gu, in1_d, in2_gu, in2_d, sum_gu, sum_d, own_gu, own_d, norms, tile) = rest[17:29]
    load_sem, send_gu, recv_gu, send_d, recv_d, norm_send, norm_recv, keep_sem = rest[29:]
    me = lax.axis_index("dp")
    row, col = lax.div(me, side), lax.rem(me, side)
    cols = loc_gu.shape[-1]
    width = cols // PIECES // QUARTERS

    loads = []
    for l in range(layers):
        g, u, d = grads[3 * l : 3 * l + 3]
        loads.append([
            pltpu.make_async_copy(src, dst, load_sem.at[l, k])
            for k, (src, dst) in enumerate(((g, loc_gu.at[0, l]), (u, loc_gu.at[1, l]), (d, loc_d.at[l])))
        ])
    for some in loads:
        for one in some:
            one.start()

    barrier = pltpu.get_barrier_semaphore()

    def greet(k, _):
        pl.semaphore_signal(barrier, inc=1, device_id={"dp": lax.rem(me + k, n)}, device_id_type=MESH)
        return _

    lax.fori_loop(1, n, greet, 0)
    pl.semaphore_wait(barrier, n - 1)

    def place(q):
        return (row, col) if q < 2 else (col, row)

    def device(q, u, v):
        u, v = lax.rem(u + 2 * side, side), lax.rem(v + 2 * side, side)
        return {"dp": u * side + v if q < 2 else v * side + u}

    def sign(q):
        return 1 if q % 2 == 0 else -1

    def wrap(k):
        return lax.rem(k + 2 * side, side)

    def lanes(h, q):
        return pl.ds(pl.multiple_of((h * QUARTERS + q) * width, 128), width)

    def strip(q):
        return pl.ds(q * (loc_d.shape[3] // QUARTERS), loc_d.shape[3] // QUARTERS)

    def sems(l, h, q, s):
        if h is None:
            return send_d.at[l, q, s], recv_d.at[l, q, s]
        return send_gu.at[l, h, q, s], recv_gu.at[l, h, q, s]

    def local_unit(l, h, q, u):
        if h is None:
            return loc_d.at[l, u, :, strip(q)] if q < 2 else loc_d.at[l, :, u, strip(q)]
        at = lanes(h, q)
        return loc_gu.at[:, l, u, :, :, at] if q < 2 else loc_gu.at[:, l, :, u, :, at]

    def local_value(l, h, q, u, v):
        a, b = (u, v) if q < 2 else (v, u)
        if h is None:
            return loc_d[l, a, b, strip(q)]
        return loc_gu[:, l, a, b, :, lanes(h, q)]

    def first(l, h, q, s):
        mu, mv = place(q)
        g = sign(q)
        dst = in1_d.at[l, q, s] if h is None else in1_gu.at[l, h, q, s]
        if s == 0:
            src = local_unit(l, h, q, wrap(mu - g))
        else:
            src = in1_d.at[l, q, s - 1] if h is None else in1_gu.at[l, h, q, s - 1]
        a, b = sems(l, h, q, s)
        return pltpu.make_async_remote_copy(src, dst, a, b, device_id=device(q, mu + g, mv), device_id_type=MESH)

    def second(l, h, q, s):
        mu, mv = place(q)
        g = sign(q)
        dst = in2_d.at[l, q, s] if h is None else in2_gu.at[l, h, q, s]
        if s == 0:
            v = wrap(mv - g)
            src = in1_d.at[l, q, 2, v] if h is None else in1_gu.at[l, h, q, 2, :, v]
        else:
            src = in2_d.at[l, q, s - 1] if h is None else in2_gu.at[l, h, q, s - 1]
        a, b = sems(l, h, q, 3 + s)
        return pltpu.make_async_remote_copy(src, dst, a, b, device_id=device(q, mu, mv + g), device_id_type=MESH)

    def add_first(l, h, q, s):
        u = wrap(place(q)[0] - sign(q) * (s + 2))

        def one(v, _):
            mine = local_value(l, h, q, u, v).astype(F32)
            if h is None:
                in1_d[l, q, s, v] = (in1_d[l, q, s, v].astype(F32) + mine).astype(BF16)
            else:
                in1_gu[l, h, q, s, :, v] = (in1_gu[l, h, q, s, :, v].astype(F32) + mine).astype(BF16)
            return _

        lax.fori_loop(0, side, one, 0)

    def add_second(l, h, q, s):
        v = wrap(place(q)[1] - sign(q) * (s + 2))
        if h is None:
            total = (in2_d[l, q, s].astype(F32) + in1_d[l, q, 2, v].astype(F32)).astype(BF16)
        else:
            total = (in2_gu[l, h, q, s].astype(F32) + in1_gu[l, h, q, 2, :, v].astype(F32)).astype(BF16)
        if s < side - 2:
            if h is None:
                in2_d[l, q, s] = total
            else:
                in2_gu[l, h, q, s] = total
            return
        total = total.astype(F32)
        if h is None:
            sum_d[l, strip(q)] = total
        else:
            sum_gu[:, l, :, lanes(h, q)] = total
        square = total * total
        square = square.reshape(-1, 8, square.shape[-1]).sum(0)
        tile[...] += sum(square[:, k : k + 128] for k in range(0, square.shape[-1], 128))

    def jobs(f):
        for l in reversed(range(layers)):
            lax.fori_loop(0, PIECES, lambda h, _: (f(l, h), _)[1], 0)
            f(l, None)

    steps = side - 1
    for l in reversed(range(layers)):
        for one in loads[l]:
            one.wait()
    tile[...] = jnp.zeros_like(tile)

    def begin(l, h):
        for q in range(QUARTERS):
            first(l, h, q, 0).start()

    jobs(begin)
    for s in range(steps):
        def advance(l, h, s=s):
            for q in range(QUARTERS):
                first(l, h, q, s).wait()
                add_first(l, h, q, s)
                (first(l, h, q, s + 1) if s + 1 < steps else second(l, h, q, 0)).start()

        jobs(advance)
    for s in range(steps):
        def advance(l, h, s=s):
            for q in range(QUARTERS):
                second(l, h, q, s).wait()
                add_second(l, h, q, s)
                if s + 1 < steps:
                    second(l, h, q, s + 1).start()

        jobs(advance)

    norms[me] = tile[...]

    def share(k):
        return pltpu.make_async_remote_copy(
            tile, norms.at[me], norm_send.at[k], norm_recv.at[k], device_id={"dp": lax.rem(me + k, n)}, device_id_type=MESH)

    lax.fori_loop(1, n, lambda k, _: (share(k).start(), _)[1], 0)
    lax.fori_loop(1, n, lambda k, _: (share(k).wait(), _)[1], 0)
    total = jnp.sum(jnp.sum(norms[...], axis=0))
    factor = jnp.minimum(1.0, 0.5 * lax.rsqrt(jnp.full((1, 128), total, F32) / count + 1e-30))

    def gather(l, h, q, s):
        mu, mv = place(q)
        g = sign(q)
        if s < steps:
            v = wrap(mv - g * s)
            a, b = (mu, v) if q < 2 else (v, mu)
            dst = new_d.at[l, a, b, q] if h is None else new_gu.at[:, l, a, b, :, lanes(h, q)]
            src = dst
            if s == 0:
                src = own_d.at[l, q] if h is None else own_gu.at[:, l, :, lanes(h, q)]
            to = device(q, mu, mv + g)
        else:
            u = wrap(mu - g * (s - steps))
            if h is None:
                dst = new_d.at[l, u, :, q] if q < 2 else new_d.at[l, :, u, q]
            else:
                at = lanes(h, q)
                dst = new_gu.at[:, l, u, :, :, at] if q < 2 else new_gu.at[:, l, :, u, :, at]
            src = dst
            to = device(q, mu + g, mv)
        a, b = sems(l, h, q, s)
        return pltpu.make_async_remote_copy(src, dst, a, b, device_id=to, device_id_type=MESH)

    def keep(l, d):
        if d:
            return pltpu.make_async_copy(own_d.at[l], new_d.at[l, row, col], keep_sem.at[l, 1])
        return pltpu.make_async_copy(own_gu.at[:, l], new_gu.at[:, l, row, col], keep_sem.at[l, 0])

    for l in reversed(range(layers)):
        for h in range(PIECES):
            for q in range(QUARTERS):
                at = pl.ds((h * QUARTERS + q) * width, width)
                by = jnp.tile(factor, (1, width // 128))
                for k, (w, m, v, nm, nv) in enumerate(((w_gate, m_gate, v_gate, nm_gate, nv_gate), (w_up, m_up, v_up, nm_up, nv_up))):
                    new, nm[l, :, at], nv[l, :, at] = adamw(
                        w[l, :, at].astype(F32), m[l, :, at], v[l, :, at], sum_gu[k, l, :, at] * by)
                    own_gu[k, l, :, at] = new
                gather(l, h, q, 0).start()
        keep(l, False).start()
        turned = sum_d[l].T
        for q in range(QUARTERS):
            rows = m_down.shape[1] // QUARTERS
            at = pl.ds(q * rows, rows)
            by = jnp.tile(factor, (1, m_down.shape[2] // 128))
            new, nm_down[l, at], nv_down[l, at] = adamw(
                w_down[l, at].astype(F32), m_down[l, at], v_down[l, at], turned[q * rows : (q + 1) * rows] * by)
            own_d[l, q] = new
            gather(l, None, q, 0).start()
        keep(l, True).start()
    for l in reversed(range(layers)):
        keep(l, False).wait()
        keep(l, True).wait()
    for s in range(2 * steps):
        def advance(l, h, s=s):
            for q in range(QUARTERS):
                gather(l, h, q, s).wait()
                if s + 1 < 2 * steps:
                    gather(l, h, q, s + 1).start()

        jobs(advance)


def sync(side, grads, own, m, v):
    layers, rows, cols = m[0].shape
    deep, narrow = m[2].shape[1:]
    quarter = deep // QUARTERS
    width = cols // PIECES // QUARTERS
    n = side * side
    steps = side - 1
    count = layers * n * (2 * rows * cols + deep * narrow)
    shaped = []
    for l in range(layers):
        g, u, d = (grads[k][l] for k in range(3))
        shaped += [g.reshape(side, side, rows, cols), u.reshape(side, side, rows, cols), d.reshape(side, side, narrow, deep)]
    vmem, hbm = pl.BlockSpec(memory_space=pltpu.VMEM), pl.BlockSpec(memory_space=pl.ANY)
    outs = pl.pallas_call(
        functools.partial(sync_kernel, side, layers, count),
        out_shape=[
            jax.ShapeDtypeStruct((2, layers, side, side, rows, cols), BF16),
            jax.ShapeDtypeStruct((layers, side, side, QUARTERS, quarter, narrow), BF16),
            *(jax.ShapeDtypeStruct(t.shape, F32) for t in (*m, *v)),
        ],
        in_specs=[hbm] * (3 * layers) + [vmem] * 9,
        out_specs=[hbm] * 2 + [vmem] * 6,
        scratch_shapes=[
            pltpu.VMEM((2, layers, side, side, rows, cols), BF16),
            pltpu.VMEM((layers, side, side, narrow, deep), BF16),
            pltpu.VMEM((layers, PIECES, QUARTERS, steps, 2, side, rows, width), BF16),
            pltpu.VMEM((layers, QUARTERS, steps, side, narrow // QUARTERS, deep), BF16),
            pltpu.VMEM((layers, PIECES, QUARTERS, steps, 2, rows, width), BF16),
            pltpu.VMEM((layers, QUARTERS, steps, narrow // QUARTERS, deep), BF16),
            pltpu.VMEM((2, layers, rows, cols), F32),
            pltpu.VMEM((layers, narrow, deep), F32),
            pltpu.VMEM((2, layers, rows, cols), BF16),
            pltpu.VMEM((layers, QUARTERS, quarter, narrow), BF16),
            pltpu.VMEM((n, 8, 128), F32),
            pltpu.VMEM((8, 128), F32),
            pltpu.SemaphoreType.DMA((layers, 3)),
            pltpu.SemaphoreType.DMA((layers, PIECES, QUARTERS, 2 * steps)),
            pltpu.SemaphoreType.DMA((layers, PIECES, QUARTERS, 2 * steps)),
            pltpu.SemaphoreType.DMA((layers, QUARTERS, 2 * steps)),
            pltpu.SemaphoreType.DMA((layers, QUARTERS, 2 * steps)),
            pltpu.SemaphoreType.DMA((n,)),
            pltpu.SemaphoreType.DMA((n,)),
            pltpu.SemaphoreType.DMA((layers, 2)),
        ],
        compiler_params=pltpu.CompilerParams(collective_id=0, has_side_effects=True, vmem_limit_bytes=60 * 2**20),
    )(*shaped, *own, *m, *v)
    gu = outs[0].reshape(2, layers, n * rows, cols)
    return (gu[0], gu[1], outs[1].reshape(layers, n * deep, narrow), *outs[2:])


def gradients(x, dy, layers, wide):
    (first, second) = layers
    a0, a0t, h1, a1, a1t, dyt = forward(x, dy, *first)
    g1, u1, d1, dh, dht = backward(True, h1, a1, a1t, dy, dyt, *second, wide=wide)
    return backward(False, a0, a0t, dh, dht, *first, wide=wide), (g1, u1, d1)


def solution(mesh):
    side = math.isqrt(mesh.shape["dp"])

    def step(x, dy, *arrays):
        weights, m, v = (arrays[i : i + 3] for i in (0, 3, 6))
        layers = weights[0].shape[0]

        by = gradients(x[0], dy[0], [tuple(w[l] for w in weights) for l in range(layers)], m[2].shape[1])
        grads = [[by[l][k] for l in range(layers)] for k in range(3)]
        me = lax.axis_index("dp")
        own = [lax.dynamic_slice_in_dim(w, me * t.shape[1], t.shape[1], 1) for w, t in zip(weights, m, strict=True)]
        return sync(side, grads, own, m, v)

    whole, block = P(None, None, None), P(None, "dp", None)
    return jax.shard_map(
        step,
        mesh=mesh,
        in_specs=(P(("rep", "dp"), None, None),) * 2 + (whole,) * 3 + (block,) * 6,
        out_specs=(P("rep", None, None),) * 3 + (P("rep", "dp", None),) * 6,
        check_vma=False,
    )
```

```python
import functools
import math

import jax
import jax.numpy as jnp
from jax import lax
from jax.experimental import pallas as pl
from jax.experimental.pallas import tpu as pltpu
from jax.sharding import PartitionSpec as P

MESH = pl.DeviceIdType.MESH
F32, BF16 = jnp.float32, jnp.bfloat16
QUARTERS = 4
PIECES = 2
CHUNKS = 4
TILE = 512


NT = (((1,), (1,)), ((), ()))

def dot(a, b): return jnp.dot(a, b, preferred_element_type=F32)
def dot_nt(a, b): return lax.dot_general(a, b, NT, preferred_element_type=F32)

def normed(h):
    wide = h.astype(F32)
    scale = lax.rsqrt(jnp.mean(wide**2, -1, keepdims=True) + 1e-6)
    return (wide * scale).astype(BF16)

def forward_kernel(x, dy, wg, wu, wd, a0, a0t, h1, a1, a1t, dyt):
    a = normed(x[...])
    a0[...] = a
    a0t[...] = a.T
    dyt[...] = dy[...].T
    gate = dot(a, wg[...])
    up = dot(a, wu[...])
    p = (jax.nn.silu(gate) * up).astype(BF16)
    h = x[...] + dot(p, wd[...]).astype(BF16)
    h1[...] = h
    b = normed(h)
    a1[...] = b
    a1t[...] = b.T

def forward(x, dy, wg, wu, wd, T=256):
    n, d = x.shape
    f = wg.shape[2]
    tile = pl.BlockSpec((T, d), lambda i: (i, 0))
    tilet = pl.BlockSpec((d, T), lambda i: (0, i))
    const = lambda s: pl.BlockSpec((None, *s), lambda i: (0, 0, 0), pipeline_mode=pl.Buffered(1))
    S = jax.ShapeDtypeStruct
    return pl.pallas_call(
        forward_kernel, grid=(n // T,),
        in_specs=[tile, tile, const((d, f)), const((d, f)), const((f, d))],
        out_specs=[tile, tilet, tile, tile, tilet, tilet],
        out_shape=[S((n, d), BF16), S((d, n), BF16), S((n, d), BF16), S((n, d), BF16), S((d, n), BF16), S((d, n), BF16)],
        compiler_params=pltpu.CompilerParams(vmem_limit_bytes=60 * 2**20),
        name="fwd",
    )(x, dy, wg, wu, wd)


def tile_step(a, dy, wg, wu, wd):
    gate = dot(a, wg)
    up = dot(a, wu)
    dp = dot_nt(dy, wd).astype(BF16).astype(F32)
    s = jax.nn.sigmoid(gate)
    act = gate * s
    p = (act * up).astype(BF16)
    du = (dp * act).astype(BF16)
    dg = (dp * up * (s + act * (1.0 - s))).astype(BF16)
    return p, dg, du

def norm_back(h, da, dy):
    wide = h.astype(F32)
    d = h.shape[-1]
    scale = lax.rsqrt(jnp.mean(wide**2, -1, keepdims=True) + 1e-6)
    along = jnp.sum(da * wide, -1, keepdims=True)
    back = da * scale - wide * (along * (scale * scale * scale) * (1.0 / d))
    return (dy.astype(F32) + back.astype(BF16).astype(F32)).astype(BF16)

def adamw(w, m, v, g):
    m = 0.9 * m + 0.1 * g
    v = 0.95 * v + 0.05 * g * g
    step = m * lax.rsqrt(v + 1e-8) + 0.1 * w
    return (w - 0.02 * step).astype(BF16), m, v


class Torus:
    def __init__(self, side):
        self.side, self.n = side, side * side
        self.me = lax.axis_index("dp")
        self.row, self.col = lax.div(self.me, side), lax.rem(self.me, side)

    def greet(self):
        barrier = pltpu.get_barrier_semaphore()

        def one(k, _):
            pl.semaphore_signal(barrier, inc=1, device_id={"dp": lax.rem(self.me + k, self.n)}, device_id_type=MESH)
            return _

        lax.fori_loop(1, self.n, one, 0)
        pl.semaphore_wait(barrier, self.n - 1)

    def place(self, q):
        return (self.row, self.col) if q < 2 else (self.col, self.row)

    def wrap(self, k):
        return lax.rem(k + 2 * self.side, self.side)

    def device(self, q, u, v):
        u, v = self.wrap(u), self.wrap(v)
        return {"dp": u * self.side + v if q < 2 else v * self.side + u}

    def sign(self, q):
        return 1 if q % 2 == 0 else -1


def backward_kernel(side, layers, *refs):
    h1, a1, a1t, dy, dyt, a0, a0t, wg, wu, wd, sum_gu, sum_d, squares = refs[:13]
    (A, AT, DY, DYT, wgb, wub, wdb, ps, gs, us, das, loc_gu, loc_d, in1_gu, in1_d, in2_gu, in2_d, norms, tile) = refs[13:32]
    act_sem, w_sem, send_gu, recv_gu, send_d, recv_d, norm_send, norm_recv = refs[32:]
    here = Torus(side)
    place, wrap, device, sign = here.place, here.wrap, here.device, here.sign
    n, d = A.shape
    F = wgb.shape[2]
    T = TILE
    width = F // QUARTERS
    steps = side - 1
    last = layers - 1

    def weights(k):
        l, c, slot = last - lax.div(k, CHUNKS), lax.rem(k, CHUNKS), lax.rem(k, 2)
        cs = pl.ds(pl.multiple_of(c * F, F), F)
        return [
            pltpu.make_async_copy(wg.at[l, :, cs], wgb.at[slot], w_sem.at[slot, 0]),
            pltpu.make_async_copy(wu.at[l, :, cs], wub.at[slot], w_sem.at[slot, 1]),
            pltpu.make_async_copy(wd.at[l, cs], wdb.at[slot], w_sem.at[slot, 2]),
        ]

    loads = [pltpu.make_async_copy(x, y, act_sem.at[k]) for k, (x, y) in enumerate(((a1, A), (dy, DY), (a1t, AT), (dyt, DYT)))]
    for one in (loads[0], loads[1], *weights(0), loads[2], loads[3]):
        one.start()
    here.greet()
    tile[...] = jnp.zeros_like(tile)
    das[...] = jnp.zeros_like(das)
    for one in loads:
        one.wait()

    def strip(q):
        return pl.ds(q * (d // QUARTERS), d // QUARTERS)

    def lanes(k, q):
        return pl.ds(pl.multiple_of((lax.rem(k, CHUNKS) * QUARTERS + q) * width, 128), width)

    def sems(gu, k, q, s):
        return (send_gu.at[k, q, s], recv_gu.at[k, q, s]) if gu else (send_d.at[k, q, s], recv_d.at[k, q, s])

    def local_unit(gu, k, q, u):
        if not gu:
            return loc_d.at[k, u, :, strip(q)] if q < 2 else loc_d.at[k, :, u, strip(q)]
        return loc_gu.at[:, u, :, :, lanes(k, q)] if q < 2 else loc_gu.at[:, :, u, :, lanes(k, q)]

    def first(gu, k, q, s):
        mu, mv = place(q)
        g = sign(q)
        ins = in1_gu if gu else in1_d
        src = local_unit(gu, k, q, wrap(mu - g)) if s == 0 else ins.at[k, q, s - 1]
        a, b = sems(gu, k, q, s)
        return pltpu.make_async_remote_copy(src, ins.at[k, q, s], a, b, device_id=device(q, mu + g, mv), device_id_type=MESH)

    def second(gu, k, q, s):
        mu, mv = place(q)
        g = sign(q)
        ins = in2_gu if gu else in2_d
        if s == 0:
            v = wrap(mv - g)
            src = in1_gu.at[k, q, steps - 1, :, v] if gu else in1_d.at[k, q, steps - 1, v]
        else:
            src = ins.at[k, q, s - 1]
        a, b = sems(gu, k, q, steps + s)
        return pltpu.make_async_remote_copy(src, ins.at[k, q, s], a, b, device_id=device(q, mu, mv + g), device_id_type=MESH)

    def add_first(gu, k, q, s):
        u = wrap(place(q)[0] - sign(q) * (s + 2))

        def one(v, _):
            a, b = (u, v) if q < 2 else (v, u)
            if gu:
                mine = loc_gu[:, a, b, :, lanes(k, q)].astype(F32)
                in1_gu[k, q, s, :, v] = (in1_gu[k, q, s, :, v].astype(F32) + mine).astype(BF16)
            else:
                mine = loc_d[k, a, b, strip(q)].astype(F32)
                in1_d[k, q, s, v] = (in1_d[k, q, s, v].astype(F32) + mine).astype(BF16)
            return _

        lax.fori_loop(0, side, one, 0)

    def add_second(gu, k, q, s):
        v = wrap(place(q)[1] - sign(q) * (s + 2))
        if gu:
            total = (in2_gu[k, q, s].astype(F32) + in1_gu[k, q, steps - 1, :, v].astype(F32)).astype(BF16)
        else:
            total = (in2_d[k, q, s].astype(F32) + in1_d[k, q, steps - 1, v].astype(F32)).astype(BF16)
        if s < steps - 1:
            if gu:
                in2_gu[k, q, s] = total
            else:
                in2_d[k, q, s] = total
            return
        total = total.astype(F32)
        if gu:
            sum_gu[:, last - lax.div(k, CHUNKS), :, lanes(k, q)] = total
        else:
            sum_d[k, strip(q)] = total
        square = total * total
        square = square.reshape(-1, 8, square.shape[-1]).sum(0)
        tile[...] += sum(square[:, i : i + 128] for i in range(0, square.shape[-1], 128))

    def begin(gu, k):
        for q in range(QUARTERS):
            first(gu, k, q, 0).start()

    def advance(gu, k, s):
        for q in range(QUARTERS):
            if s < steps:
                first(gu, k, q, s).wait()
                add_first(gu, k, q, s)
                (first(gu, k, q, s + 1) if s + 1 < steps else second(gu, k, q, 0)).start()
            else:
                second(gu, k, q, s - steps).wait()
                add_second(gu, k, q, s - steps)
                if s + 1 < 2 * steps:
                    second(gu, k, q, s - steps + 1).start()

    def chunk(k, inner):
        slot, c = lax.rem(k, 2), lax.rem(k, CHUNKS)
        for one in weights(k):
            one.wait()

        @pl.when(k + 1 < layers * CHUNKS)
        def _():
            for one in weights(k + 1):
                one.start()

        def ticks(s):
            for back, more in ((1, 0), (2, steps)):
                if inner:
                    pl.when(k >= back)(lambda: advance(True, k - back, s + more))
                else:
                    advance(True, k - back, s + more)

        for t in range(n // T):
            ts = pl.ds(t * T, T)
            p, dg, du = tile_step(A[ts], DY[ts], wgb[slot], wub[slot], wdb[slot])
            ps[ts] = p
            gs[ts] = dg
            us[ts] = du
            if inner:
                das[ts] += dot_nt(dg, wgb[slot]) + dot_nt(du, wub[slot])
            if t % 2 == 1:
                ticks(t // 2)
        cs = pl.ds(pl.multiple_of(c * F, F), F)
        rows = loc_gu.shape[3]
        for which, of in ((0, gs), (1, us)):
            g = dot(AT[...], of[...]).astype(BF16)
            for i in range(side * side):
                loc_gu[which, i // side, i % side, :, cs] = g[i * rows : (i + 1) * rows]
        l = last - lax.div(k, CHUNKS)
        g = dot(DYT[...], ps[...]).astype(BF16)
        wide = loc_d.shape[4]
        for i in range(F // wide):
            to = c * (F // wide) + i
            loc_d[l, lax.div(to, side), lax.rem(to, side)] = g[:, i * wide : (i + 1) * wide]
        ticks(steps - 1)
        begin(True, k)

    lax.fori_loop(0, CHUNKS, lambda k, _: (chunk(k, True), _)[1], 0)
    begin(False, last)

    again = [pltpu.make_async_copy(x, y, act_sem.at[k]) for k, (x, y) in enumerate(((h1, A), (a0, A), (a0t, AT)))]
    again[0].start()
    again[2].start()
    again[0].wait()

    def turn(t, _):
        ts = pl.ds(pl.multiple_of(t * 256, 256), 256)
        r = norm_back(A[ts], das[ts].astype(BF16).astype(F32), DY[ts])
        DY[ts] = r
        DYT[:, ts] = r.T
        return _

    lax.fori_loop(0, n // 256, turn, 0)
    again[1].start()
    again[1].wait()
    again[2].wait()

    def outer(k, _):
        chunk(k, False)
        for i in range(CHUNKS):
            pl.when(k == CHUNKS + i)(lambda: advance(False, last, i))
        return _

    lax.fori_loop(CHUNKS, 2 * CHUNKS, outer, 0)
    begin(False, 0)
    end = 2 * CHUNKS - 1
    for s in range(2 * steps):
        if s < steps:
            advance(True, end - 1, steps + s)
        advance(True, end, s)
        if CHUNKS + s < 2 * steps:
            advance(False, last, CHUNKS + s)
        advance(False, 0, s)

    norms[here.me] = tile[...]

    def share(k):
        return pltpu.make_async_remote_copy(
            tile, norms.at[here.me], norm_send.at[k], norm_recv.at[k],
            device_id={"dp": lax.rem(here.me + k, here.n)}, device_id_type=MESH)

    lax.fori_loop(1, here.n, lambda k, _: (share(k).start(), _)[1], 0)
    lax.fori_loop(1, here.n, lambda k, _: (share(k).wait(), _)[1], 0)
    squares[...] = jnp.sum(norms[...], axis=0)


def backward(side, layers, acts, weights, rows, deep):
    n, d = acts[0].shape
    f = weights[0].shape[2]
    F = f // CHUNKS
    width = F // QUARTERS
    steps = side - 1
    S, V = jax.ShapeDtypeStruct, pltpu.VMEM
    jobs = layers * CHUNKS
    vmem, hbm = pl.BlockSpec(memory_space=pltpu.VMEM), pl.BlockSpec(memory_space=pl.ANY)
    return pl.pallas_call(
        functools.partial(backward_kernel, side, layers),
        out_shape=[S((2, layers, rows, f), F32), S((layers, d, deep), F32), S((8, 128), F32)],
        in_specs=[hbm] * 10,
        out_specs=[vmem] * 3,
        scratch_shapes=[
            V((n, d), BF16), V((d, n), BF16), V((n, d), BF16), V((d, n), BF16),
            V((2, d, F), BF16), V((2, d, F), BF16), V((2, F, d), BF16),
            V((n, F), BF16), V((n, F), BF16), V((n, F), BF16), V((n, d), F32),
            V((2, side, side, rows, f), BF16),
            V((layers, side, side, d, deep), BF16),
            V((jobs, QUARTERS, steps, 2, side, rows, width), BF16),
            V((layers, QUARTERS, steps, side, d // QUARTERS, deep), BF16),
            V((jobs, QUARTERS, steps, 2, rows, width), BF16),
            V((layers, QUARTERS, steps, d // QUARTERS, deep), BF16),
            V((side * side, 8, 128), F32), V((8, 128), F32),
            pltpu.SemaphoreType.DMA((4,)),
            pltpu.SemaphoreType.DMA((2, 3)),
            pltpu.SemaphoreType.DMA((jobs, QUARTERS, 2 * steps)),
            pltpu.SemaphoreType.DMA((jobs, QUARTERS, 2 * steps)),
            pltpu.SemaphoreType.DMA((layers, QUARTERS, 2 * steps)),
            pltpu.SemaphoreType.DMA((layers, QUARTERS, 2 * steps)),
            pltpu.SemaphoreType.DMA((side * side,)),
            pltpu.SemaphoreType.DMA((side * side,)),
        ],
        compiler_params=pltpu.CompilerParams(collective_id=0, has_side_effects=True, vmem_limit_bytes=67043328),
        name="bwd",
    )(*acts, *weights)


def gather_kernel(side, layers, count, *refs):
    sum_gu, sum_d, squares, w_gate, w_up, w_down, m_gate, m_up, m_down, v_gate, v_up, v_down = refs[:12]
    new_gu, new_d, nm_gate, nm_up, nm_down, nv_gate, nv_up, nv_down = refs[12:20]
    own_gu, own_d, old_gu, old_d, send_gu, recv_gu, send_d, recv_d, keep_sem = refs[20:]
    here = Torus(side)
    place, wrap, device, sign, me, row, col = here.place, here.wrap, here.device, here.sign, here.me, here.row, here.col
    steps = side - 1
    rows, cols = m_gate.shape[1:]
    deep = m_down.shape[1]
    width = cols // PIECES // QUARTERS
    at, deep_at = pl.ds(pl.multiple_of(me * rows, 8), rows), pl.ds(pl.multiple_of(me * deep, 8), deep)
    olds = [
        pltpu.make_async_copy(w_gate.at[:, at], old_gu.at[0], keep_sem.at[0, 0]),
        pltpu.make_async_copy(w_up.at[:, at], old_gu.at[1], keep_sem.at[0, 1]),
        pltpu.make_async_copy(w_down.at[:, deep_at], old_d, keep_sem.at[1, 0]),
    ]
    for one in olds:
        one.start()
    here.greet()
    for one in olds:
        one.wait()

    def lanes(h, q):
        return pl.ds(pl.multiple_of((h * QUARTERS + q) * width, 128), width)

    def sems(l, h, q, s):
        if h is None:
            return send_d.at[l, q, s], recv_d.at[l, q, s]
        return send_gu.at[l, h, q, s], recv_gu.at[l, h, q, s]

    def jobs(f):
        for l in reversed(range(layers)):
            lax.fori_loop(0, PIECES, lambda h, _: (f(l, h), _)[1], 0)
            f(l, None)

    total = jnp.sum(squares[...])
    factor = jnp.minimum(1.0, 0.5 * lax.rsqrt(jnp.full((1, 128), total, F32) / count + 1e-30))

    def gather(l, h, q, s):
        mu, mv = place(q)
        g = sign(q)
        if s < steps:
            v = wrap(mv - g * s)
            a, b = (mu, v) if q < 2 else (v, mu)
            dst = new_d.at[l, a, b, q] if h is None else new_gu.at[:, l, a, b, :, lanes(h, q)]
            src = dst
            if s == 0:
                src = own_d.at[l, q] if h is None else own_gu.at[:, l, :, lanes(h, q)]
            to = device(q, mu, mv + g)
        else:
            u = wrap(mu - g * (s - steps))
            if h is None:
                dst = new_d.at[l, u, :, q] if q < 2 else new_d.at[l, :, u, q]
            else:
                at = lanes(h, q)
                dst = new_gu.at[:, l, u, :, :, at] if q < 2 else new_gu.at[:, l, :, u, :, at]
            src = dst
            to = device(q, mu + g, mv)
        a, b = sems(l, h, q, s)
        return pltpu.make_async_remote_copy(src, dst, a, b, device_id=to, device_id_type=MESH)

    def keep(l, d):
        if d:
            return pltpu.make_async_copy(own_d.at[l], new_d.at[l, row, col], keep_sem.at[l, 1])
        return pltpu.make_async_copy(own_gu.at[:, l], new_gu.at[:, l, row, col], keep_sem.at[l, 0])

    for l in reversed(range(layers)):
        for h in range(PIECES):
            for q in range(QUARTERS):
                at = pl.ds((h * QUARTERS + q) * width, width)
                by = jnp.tile(factor, (1, width // 128))
                for k, (w, m, v, nm, nv) in enumerate(((old_gu.at[0], m_gate, v_gate, nm_gate, nv_gate), (old_gu.at[1], m_up, v_up, nm_up, nv_up))):
                    new, nm[l, :, at], nv[l, :, at] = adamw(
                        w[l, :, at].astype(F32), m[l, :, at], v[l, :, at], sum_gu[k, l, :, at] * by)
                    own_gu[k, l, :, at] = new
                gather(l, h, q, 0).start()
        keep(l, False).start()
        turned = sum_d[l].T
        for q in range(QUARTERS):
            rows = m_down.shape[1] // QUARTERS
            at = pl.ds(q * rows, rows)
            by = jnp.tile(factor, (1, m_down.shape[2] // 128))
            new, nm_down[l, at], nv_down[l, at] = adamw(
                old_d[l, at].astype(F32), m_down[l, at], v_down[l, at], turned[q * rows : (q + 1) * rows] * by)
            own_d[l, q] = new
            gather(l, None, q, 0).start()
        keep(l, True).start()
    for l in reversed(range(layers)):
        keep(l, False).wait()
        keep(l, True).wait()
    for s in range(2 * steps):
        def advance(l, h, s=s):
            for q in range(QUARTERS):
                gather(l, h, q, s).wait()
                if s + 1 < 2 * steps:
                    gather(l, h, q, s + 1).start()

        jobs(advance)


def gather(side, sums, w, m, v):
    layers, rows, cols = m[0].shape
    deep, narrow = m[2].shape[1:]
    quarter = deep // QUARTERS
    n = side * side
    steps = side - 1
    count = layers * n * (2 * rows * cols + deep * narrow)
    vmem, hbm = pl.BlockSpec(memory_space=pltpu.VMEM), pl.BlockSpec(memory_space=pl.ANY)
    outs = pl.pallas_call(
        functools.partial(gather_kernel, side, layers, count),
        out_shape=[
            jax.ShapeDtypeStruct((2, layers, side, side, rows, cols), BF16),
            jax.ShapeDtypeStruct((layers, side, side, QUARTERS, quarter, narrow), BF16),
            *(jax.ShapeDtypeStruct(t.shape, F32) for t in (*m, *v)),
        ],
        in_specs=[vmem] * 3 + [hbm] * 3 + [vmem] * 6,
        out_specs=[hbm] * 2 + [vmem] * 6,
        scratch_shapes=[
            pltpu.VMEM((2, layers, rows, cols), BF16),
            pltpu.VMEM((layers, QUARTERS, quarter, narrow), BF16),
            pltpu.VMEM((2, layers, rows, cols), BF16),
            pltpu.VMEM((layers, deep, narrow), BF16),
            pltpu.SemaphoreType.DMA((layers, PIECES, QUARTERS, 2 * steps)),
            pltpu.SemaphoreType.DMA((layers, PIECES, QUARTERS, 2 * steps)),
            pltpu.SemaphoreType.DMA((layers, QUARTERS, 2 * steps)),
            pltpu.SemaphoreType.DMA((layers, QUARTERS, 2 * steps)),
            pltpu.SemaphoreType.DMA((layers, 2)),
        ],
        compiler_params=pltpu.CompilerParams(collective_id=1, has_side_effects=True, vmem_limit_bytes=40 * 2**20),
        name="gather",
    )(*sums, *w, *m, *v)
    gu = outs[0].reshape(2, layers, n * rows, cols)
    return (gu[0], gu[1], outs[1].reshape(layers, n * deep, narrow), *outs[2:])


def solution(mesh):
    side = math.isqrt(mesh.shape["dp"])

    def step(x, dy, *arrays):
        weights, m, v = (arrays[i : i + 3] for i in (0, 3, 6))
        layers = weights[0].shape[0]

        a0, a0t, h1, a1, a1t, dyt = forward(x[0], dy[0], *weights)
        acts = (h1, a1, a1t, dy[0], dyt, a0, a0t)
        sums = backward(side, weights[0].shape[0], acts, weights, m[0].shape[1], m[2].shape[1])
        return gather(side, sums, weights, m, v)

    whole, block = P(None, None, None), P(None, "dp", None)
    return jax.shard_map(
        step,
        mesh=mesh,
        in_specs=(P(("rep", "dp"), None, None),) * 2 + (whole,) * 3 + (block,) * 6,
        out_specs=(P("rep", None, None),) * 3 + (P("rep", "dp", None),) * 6,
        check_vma=False,
    )
```

```python
import functools
import math

import jax
import jax.numpy as jnp
from jax import lax
from jax.experimental import pallas as pl
from jax.experimental.pallas import tpu as pltpu
from jax.sharding import PartitionSpec as P

MESH = pl.DeviceIdType.MESH
F32, BF16 = jnp.float32, jnp.bfloat16
QUARTERS = 4
PIECES = 2
CHUNKS = 4
TILE = 512
STEPS_AT = (((3, 3), (2, 1)), ((3, 4), (1, 0)), ((3, 5), (2, 2)))


NT = (((1,), (1,)), ((), ()))

def dot(a, b): return jnp.dot(a, b, preferred_element_type=F32)
def dot_nt(a, b): return lax.dot_general(a, b, NT, preferred_element_type=F32)

def normed(h):
    wide = h.astype(F32)
    scale = lax.rsqrt(jnp.mean(wide**2, -1, keepdims=True) + 1e-6)
    return (wide * scale).astype(BF16)

def forward_kernel(x, dy, wg, wu, wd, a0, a0t, h1, a1, a1t, dyt):
    a = normed(x[...])
    a0[...] = a
    a0t[...] = a.T
    dyt[...] = dy[...].T
    gate = dot(a, wg[...])
    up = dot(a, wu[...])
    p = (jax.nn.silu(gate) * up).astype(BF16)
    h = x[...] + dot(p, wd[...]).astype(BF16)
    h1[...] = h
    b = normed(h)
    a1[...] = b
    a1t[...] = b.T

def forward(x, dy, wg, wu, wd, T=256):
    n, d = x.shape
    f = wg.shape[2]
    tile = pl.BlockSpec((T, d), lambda i: (i, 0))
    tilet = pl.BlockSpec((d, T), lambda i: (0, i))
    const = lambda s: pl.BlockSpec((None, *s), lambda i: (0, 0, 0), pipeline_mode=pl.Buffered(1))
    S = jax.ShapeDtypeStruct
    return pl.pallas_call(
        forward_kernel, grid=(n // T,),
        in_specs=[tile, tile, const((d, f)), const((d, f)), const((f, d))],
        out_specs=[tile, tilet, tile, tile, tilet, tilet],
        out_shape=[S((n, d), BF16), S((d, n), BF16), S((n, d), BF16), S((n, d), BF16), S((d, n), BF16), S((d, n), BF16)],
        compiler_params=pltpu.CompilerParams(vmem_limit_bytes=60 * 2**20),
        name="fwd",
    )(x, dy, wg, wu, wd)


def tile_step(a, dy, wg, wu, wd):
    gate = dot(a, wg)
    up = dot(a, wu)
    dp = dot_nt(dy, wd).astype(BF16).astype(F32)
    s = jax.nn.sigmoid(gate)
    act = gate * s
    p = (act * up).astype(BF16)
    du = (dp * act).astype(BF16)
    dg = (dp * up * (s + act * (1.0 - s))).astype(BF16)
    return p, dg, du

def norm_back(h, da, dy):
    wide = h.astype(F32)
    d = h.shape[-1]
    scale = lax.rsqrt(jnp.mean(wide**2, -1, keepdims=True) + 1e-6)
    along = jnp.sum(da * wide, -1, keepdims=True)
    back = da * scale - wide * (along * (scale * scale * scale) * (1.0 / d))
    return (dy.astype(F32) + back.astype(BF16).astype(F32)).astype(BF16)

def adamw(w, m, v, g):
    m = 0.9 * m + 0.1 * g
    v = 0.95 * v + 0.05 * g * g
    step = m * lax.rsqrt(v + 1e-8) + 0.1 * w
    return (w - 0.02 * step).astype(BF16), m, v


class Torus:
    def __init__(self, side):
        self.side, self.n = side, side * side
        self.me = lax.axis_index("dp")
        self.row, self.col = lax.div(self.me, side), lax.rem(self.me, side)

    def greet(self):
        barrier = pltpu.get_barrier_semaphore()

        def one(k, _):
            pl.semaphore_signal(barrier, inc=1, device_id={"dp": lax.rem(self.me + k, self.n)}, device_id_type=MESH)
            return _

        lax.fori_loop(1, self.n, one, 0)
        pl.semaphore_wait(barrier, self.n - 1)

    def place(self, q):
        return (self.row, self.col) if q < 2 else (self.col, self.row)

    def wrap(self, k):
        return lax.rem(k + 2 * self.side, self.side)

    def device(self, q, u, v):
        u, v = self.wrap(u), self.wrap(v)
        return {"dp": u * self.side + v if q < 2 else v * self.side + u}

    def sign(self, q):
        return 1 if q % 2 == 0 else -1


def backward_kernel(side, layers, *refs):
    h1, a1, a1t, dy, dyt, a0, a0t, wg, wu, wd, sum_gu, sum_d, squares = refs[:13]
    (A, AT, DY, DYT, wgb, wub, wdb, ps, gs, us, das, loc_gu, loc_d, in1_gu, in1_d, in2_gu, in2_d, norms, tile) = refs[13:32]
    act_sem, w_sem, send_gu, recv_gu, send_d, recv_d, norm_send, norm_recv = refs[32:]
    here = Torus(side)
    place, wrap, device, sign = here.place, here.wrap, here.device, here.sign
    n, d = A.shape
    F = wgb.shape[2]
    T = TILE
    width = F // QUARTERS
    steps = side - 1
    last = layers - 1

    def weights(k):
        l, c, slot = last - lax.div(k, CHUNKS), lax.rem(k, CHUNKS), lax.rem(k, 2)
        cs = pl.ds(pl.multiple_of(c * F, F), F)
        return [
            pltpu.make_async_copy(wg.at[l, :, cs], wgb.at[slot], w_sem.at[slot, 0]),
            pltpu.make_async_copy(wu.at[l, :, cs], wub.at[slot], w_sem.at[slot, 1]),
            pltpu.make_async_copy(wd.at[l, cs], wdb.at[slot], w_sem.at[slot, 2]),
        ]

    loads = [pltpu.make_async_copy(x, y, act_sem.at[k]) for k, (x, y) in enumerate(((a1, A), (dy, DY), (a1t, AT), (dyt, DYT)))]
    for one in (loads[0], loads[1], *weights(0), loads[2], loads[3]):
        one.start()
    here.greet()
    tile[...] = jnp.zeros_like(tile)
    das[...] = jnp.zeros_like(das)
    for one in loads[:2]:
        one.wait()

    def strip(q):
        return pl.ds(q * (d // QUARTERS), d // QUARTERS)

    def lanes(k, q):
        return pl.ds(pl.multiple_of((lax.rem(k, CHUNKS) * QUARTERS + q) * width, 128), width)

    def sems(gu, k, q, s):
        return (send_gu.at[k, q, s], recv_gu.at[k, q, s]) if gu else (send_d.at[k, q, s], recv_d.at[k, q, s])

    def local_unit(gu, k, q, u):
        if not gu:
            return loc_d.at[k, u, :, strip(q)] if q < 2 else loc_d.at[k, :, u, strip(q)]
        return loc_gu.at[:, u, :, :, lanes(k, q)] if q < 2 else loc_gu.at[:, :, u, :, lanes(k, q)]

    def first(gu, k, q, s):
        mu, mv = place(q)
        g = sign(q)
        ins = in1_gu if gu else in1_d
        src = local_unit(gu, k, q, wrap(mu - g)) if s == 0 else ins.at[k, q, s - 1]
        a, b = sems(gu, k, q, s)
        return pltpu.make_async_remote_copy(src, ins.at[k, q, s], a, b, device_id=device(q, mu + g, mv), device_id_type=MESH)

    def second(gu, k, q, s):
        mu, mv = place(q)
        g = sign(q)
        ins = in2_gu if gu else in2_d
        if s == 0:
            v = wrap(mv - g)
            src = in1_gu.at[k, q, steps - 1, :, v] if gu else in1_d.at[k, q, steps - 1, v]
        else:
            src = ins.at[k, q, s - 1]
        a, b = sems(gu, k, q, steps + s)
        return pltpu.make_async_remote_copy(src, ins.at[k, q, s], a, b, device_id=device(q, mu, mv + g), device_id_type=MESH)

    def add_first(gu, k, q, s):
        u = wrap(place(q)[0] - sign(q) * (s + 2))

        def one(v, _):
            a, b = (u, v) if q < 2 else (v, u)
            if gu:
                mine = loc_gu[:, a, b, :, lanes(k, q)].astype(F32)
                in1_gu[k, q, s, :, v] = (in1_gu[k, q, s, :, v].astype(F32) + mine).astype(BF16)
            else:
                mine = loc_d[k, a, b, strip(q)].astype(F32)
                in1_d[k, q, s, v] = (in1_d[k, q, s, v].astype(F32) + mine).astype(BF16)
            return _

        lax.fori_loop(0, side, one, 0)

    def add_second(gu, k, q, s):
        v = wrap(place(q)[1] - sign(q) * (s + 2))
        if gu:
            total = (in2_gu[k, q, s].astype(F32) + in1_gu[k, q, steps - 1, :, v].astype(F32)).astype(BF16)
        else:
            total = (in2_d[k, q, s].astype(F32) + in1_d[k, q, steps - 1, v].astype(F32)).astype(BF16)
        if s < steps - 1:
            if gu:
                in2_gu[k, q, s] = total
            else:
                in2_d[k, q, s] = total
            return
        total = total.astype(F32)
        if gu:
            sum_gu[:, last - lax.div(k, CHUNKS), :, lanes(k, q)] = total
        else:
            sum_d[k, strip(q)] = total
        square = total * total
        square = square.reshape(-1, 8, square.shape[-1]).sum(0)
        tile[...] += sum(square[:, i : i + 128] for i in range(0, square.shape[-1], 128))

    def begin(gu, k):
        for q in range(QUARTERS):
            first(gu, k, q, 0).start()

    def advance(gu, k, s):
        for q in range(QUARTERS):
            if s < steps:
                first(gu, k, q, s).wait()
                add_first(gu, k, q, s)
                (first(gu, k, q, s + 1) if s + 1 < steps else second(gu, k, q, 0)).start()
            else:
                second(gu, k, q, s - steps).wait()
                add_second(gu, k, q, s - steps)
                if s + 1 < 2 * steps:
                    second(gu, k, q, s - steps + 1).start()

    def chunk(k, inner):
        slot, c = lax.rem(k, 2), lax.rem(k, CHUNKS)
        for one in weights(k):
            one.wait()

        @pl.when(k + 1 < layers * CHUNKS)
        def _():
            for one in weights(k + 1):
                one.start()

        def ticks(point):
            for back, step in STEPS_AT[point]:
                if inner:
                    pl.when(k >= back)(lambda: advance(True, k - back, step))
                else:
                    advance(True, k - back, step)

        for t in range(n // T):
            ts = pl.ds(t * T, T)
            p, dg, du = tile_step(A[ts], DY[ts], wgb[slot], wub[slot], wdb[slot])
            ps[ts] = p
            gs[ts] = dg
            us[ts] = du
            if inner:
                das[ts] += dot_nt(dg, wgb[slot]) + dot_nt(du, wub[slot])
            if t % 2 == 1:
                ticks(t // 2)
        if inner:
            @pl.when(k == 0)
            def _():
                for one in loads[2:]:
                    one.wait()

        cs = pl.ds(pl.multiple_of(c * F, F), F)
        rows = loc_gu.shape[3]
        for which, of in ((0, gs), (1, us)):
            g = dot(AT[...], of[...]).astype(BF16)
            for i in range(side * side):
                loc_gu[which, i // side, i % side, :, cs] = g[i * rows : (i + 1) * rows]
        l = last - lax.div(k, CHUNKS)
        g = dot(DYT[...], ps[...]).astype(BF16)
        wide = loc_d.shape[4]
        for i in range(F // wide):
            to = c * (F // wide) + i
            loc_d[l, lax.div(to, side), lax.rem(to, side)] = g[:, i * wide : (i + 1) * wide]
        ticks(2)
        begin(True, k)

    lax.fori_loop(0, CHUNKS, lambda k, _: (chunk(k, True), _)[1], 0)
    begin(False, last)

    again = [pltpu.make_async_copy(x, y, act_sem.at[k]) for k, (x, y) in enumerate(((h1, A), (a0, A), (a0t, AT)))]
    again[0].start()
    again[2].start()
    again[0].wait()

    def turn(t, _):
        ts = pl.ds(pl.multiple_of(t * 256, 256), 256)
        r = norm_back(A[ts], das[ts].astype(BF16).astype(F32), DY[ts])
        DY[ts] = r
        DYT[:, ts] = r.T
        return _

    lax.fori_loop(0, n // 256, turn, 0)
    again[1].start()
    again[1].wait()
    again[2].wait()

    def outer(k, _):
        chunk(k, False)
        for i in range(CHUNKS):
            pl.when(k == CHUNKS + i)(lambda: advance(False, last, i))
        return _

    lax.fori_loop(CHUNKS, 2 * CHUNKS, outer, 0)
    begin(False, 0)
    end = 2 * CHUNKS - 1
    for s in range(2 * steps):
        for gu, k, done in ((True, end - 2, 3), (False, last, CHUNKS), (True, end - 1, 1), (True, end, 0), (False, 0, 0)):
            if done + s < 2 * steps:
                advance(gu, k, done + s)

    norms[here.me] = tile[...]

    def share(k):
        return pltpu.make_async_remote_copy(
            tile, norms.at[here.me], norm_send.at[k], norm_recv.at[k],
            device_id={"dp": lax.rem(here.me + k, here.n)}, device_id_type=MESH)

    lax.fori_loop(1, here.n, lambda k, _: (share(k).start(), _)[1], 0)
    lax.fori_loop(1, here.n, lambda k, _: (share(k).wait(), _)[1], 0)
    squares[...] = jnp.sum(norms[...], axis=0)


def backward(side, layers, acts, weights, rows, deep):
    n, d = acts[0].shape
    f = weights[0].shape[2]
    F = f // CHUNKS
    width = F // QUARTERS
    steps = side - 1
    S, V = jax.ShapeDtypeStruct, pltpu.VMEM
    jobs = layers * CHUNKS
    vmem, hbm = pl.BlockSpec(memory_space=pltpu.VMEM), pl.BlockSpec(memory_space=pl.ANY)
    return pl.pallas_call(
        functools.partial(backward_kernel, side, layers),
        out_shape=[S((2, layers, rows, f), F32), S((layers, d, deep), F32), S((8, 128), F32)],
        in_specs=[hbm] * 10,
        out_specs=[vmem] * 3,
        scratch_shapes=[
            V((n, d), BF16), V((d, n), BF16), V((n, d), BF16), V((d, n), BF16),
            V((2, d, F), BF16), V((2, d, F), BF16), V((2, F, d), BF16),
            V((n, F), BF16), V((n, F), BF16), V((n, F), BF16), V((n, d), F32),
            V((2, side, side, rows, f), BF16),
            V((layers, side, side, d, deep), BF16),
            V((jobs, QUARTERS, steps, 2, side, rows, width), BF16),
            V((layers, QUARTERS, steps, side, d // QUARTERS, deep), BF16),
            V((jobs, QUARTERS, steps, 2, rows, width), BF16),
            V((layers, QUARTERS, steps, d // QUARTERS, deep), BF16),
            V((side * side, 8, 128), F32), V((8, 128), F32),
            pltpu.SemaphoreType.DMA((4,)),
            pltpu.SemaphoreType.DMA((2, 3)),
            pltpu.SemaphoreType.DMA((jobs, QUARTERS, 2 * steps)),
            pltpu.SemaphoreType.DMA((jobs, QUARTERS, 2 * steps)),
            pltpu.SemaphoreType.DMA((layers, QUARTERS, 2 * steps)),
            pltpu.SemaphoreType.DMA((layers, QUARTERS, 2 * steps)),
            pltpu.SemaphoreType.DMA((side * side,)),
            pltpu.SemaphoreType.DMA((side * side,)),
        ],
        compiler_params=pltpu.CompilerParams(collective_id=0, has_side_effects=True, vmem_limit_bytes=67043328),
        name="bwd",
    )(*acts, *weights)


def adam_kernel(count, me, gate, up, down, sum_gu, sum_d, squares, *refs):
    m, v, own, nm, nv = refs[:3], refs[3:6], refs[6:8], refs[8:11], refs[11:]
    total = jnp.sum(squares[...])
    factor = jnp.minimum(1.0, 0.5 * lax.rsqrt(jnp.full((1, 1), total, F32) / count + 1e-30))
    for k, w in enumerate((gate, up)):
        own[0][k], nm[k][...], nv[k][...] = adamw(w[...].astype(F32), m[k][...], v[k][...], sum_gu[k] * factor)
    own[1][...], nm[2][...], nv[2][...] = adamw(down[...].astype(F32), m[2][...], v[2][...], sum_d[...].T * factor)


def adam(sums, w, m, v, n):
    layers, rows, cols = m[0].shape
    deep, narrow = m[2].shape[1:]
    S = jax.ShapeDtypeStruct
    wide, tall = (None, rows, cols), (None, deep, narrow)
    mine = lambda s: pl.BlockSpec(s, lambda l, me: (l, me[0], 0))
    whole = lambda s: pl.BlockSpec(s, lambda l, me: (l, 0, 0))
    both = pl.BlockSpec((2, None, rows, cols), lambda l, me: (0, l, 0, 0))
    moments = [whole(wide), whole(wide), whole(tall)]
    outs = pl.pallas_call(
        functools.partial(adam_kernel, layers * n * (2 * rows * cols + deep * narrow)),
        grid_spec=pltpu.PrefetchScalarGridSpec(
            num_scalar_prefetch=1,
            grid=(layers,),
            in_specs=[mine(wide), mine(wide), mine(tall), both, whole((None, narrow, deep)), pl.BlockSpec((8, 128), lambda l, me: (0, 0)), *moments, *moments],
            out_specs=[both, whole(tall), *moments, *moments],
        ),
        out_shape=[S((2, layers, rows, cols), BF16), S((layers, deep, narrow), BF16), *(S(t.shape, F32) for t in (*m, *v))],
        compiler_params=pltpu.CompilerParams(vmem_limit_bytes=62 * 2**20),
        name="adam",
    )(lax.axis_index("dp").reshape(1), *w, *sums, *m, *v)
    return outs[0], outs[1], outs[2:]


def gather_kernel(side, layers, *refs):
    own_gu, own_d = refs[:2]
    new_gu, new_d = refs[2 : 2 + layers], refs[2 + layers : 2 + 2 * layers]
    send_gu, recv_gu, send_d, recv_d = refs[2 + 2 * layers :]
    here = Torus(side)
    place, wrap, device, sign, row, col = here.place, here.wrap, here.device, here.sign, here.row, here.col
    steps = side - 1
    cols = own_gu.shape[3]
    quarter = own_d.shape[1] // QUARTERS
    width = cols // PIECES // QUARTERS
    for l in range(layers):
        new_gu[l][:, row, col] = own_gu[:, l]
        for q in range(QUARTERS):
            new_d[l][row, col, q] = own_d[l, q * quarter : (q + 1) * quarter]
    here.greet()

    def lanes(h, q):
        return pl.ds(pl.multiple_of((h * QUARTERS + q) * width, 128), width)

    def sems(l, h, q, s):
        if h is None:
            return send_d.at[l, q, s], recv_d.at[l, q, s]
        return send_gu.at[l, h, q, s], recv_gu.at[l, h, q, s]

    def jobs(f):
        for l in reversed(range(layers)):
            lax.fori_loop(0, PIECES, lambda h, _: (f(l, h), _)[1], 0)
            f(l, None)

    def gather(l, h, q, s):
        mu, mv = place(q)
        g = sign(q)
        gu, down = new_gu[l], new_d[l]
        if s < steps:
            v = wrap(mv - g * s)
            a, b = (mu, v) if q < 2 else (v, mu)
            src = dst = down.at[a, b, q] if h is None else gu.at[:, a, b, :, lanes(h, q)]
            if s == 0:
                src = own_d.at[l, pl.ds(q * quarter, quarter)] if h is None else own_gu.at[:, l, :, lanes(h, q)]
            to = device(q, mu, mv + g)
        else:
            u = wrap(mu - g * (s - steps))
            if h is None:
                dst = down.at[u, :, q] if q < 2 else down.at[:, u, q]
            else:
                dst = gu.at[:, u, :, :, lanes(h, q)] if q < 2 else gu.at[:, :, u, :, lanes(h, q)]
            src = dst
            to = device(q, mu + g, mv)
        a, b = sems(l, h, q, s)
        return pltpu.make_async_remote_copy(src, dst, a, b, device_id=to, device_id_type=MESH)

    def begin(l, h):
        for q in range(QUARTERS):
            gather(l, h, q, 0).start()

    jobs(begin)
    for s in range(2 * steps):
        def advance(l, h, s=s):
            for q in range(QUARTERS):
                gather(l, h, q, s).wait()
                if s + 1 < 2 * steps:
                    gather(l, h, q, s + 1).start()

        jobs(advance)


def gather(side, own_gu, own_d):
    layers, rows, cols = own_gu.shape[1:]
    deep, narrow = own_d.shape[1:]
    n = side * side
    steps = side - 1
    vmem = pl.BlockSpec(memory_space=pltpu.VMEM)
    S = jax.ShapeDtypeStruct
    outs = pl.pallas_call(
        functools.partial(gather_kernel, side, layers),
        out_shape=[S((2, side, side, rows, cols), BF16)] * layers + [S((side, side, QUARTERS, deep // QUARTERS, narrow), BF16)] * layers,
        in_specs=[vmem] * 2,
        out_specs=[vmem] * (2 * layers),
        scratch_shapes=[
            pltpu.SemaphoreType.DMA((layers, PIECES, QUARTERS, 2 * steps)),
            pltpu.SemaphoreType.DMA((layers, PIECES, QUARTERS, 2 * steps)),
            pltpu.SemaphoreType.DMA((layers, QUARTERS, 2 * steps)),
            pltpu.SemaphoreType.DMA((layers, QUARTERS, 2 * steps)),
        ],
        compiler_params=pltpu.CompilerParams(collective_id=1, has_side_effects=True, vmem_limit_bytes=4 * 2**20),
        name="gather",
    )(own_gu, own_d)
    gus, downs = outs[:layers], outs[layers:]
    return finish([t.reshape(2, n * rows, cols) for t in gus], [t.reshape(n * deep, narrow) for t in downs])


def finish_kernel(layers, *refs):
    gus, downs, (gate, up, down, sem) = refs[:layers], refs[layers : 2 * layers], refs[2 * layers :]
    copies = []
    for l in range(layers):
        for k, (x, y) in enumerate(((gus[l].at[0], gate), (gus[l].at[1], up), (downs[l], down))):
            copies.append(pltpu.make_async_copy(x, y.at[l], sem.at[l, k]))
    for one in copies:
        one.start()
    for one in copies:
        one.wait()


def finish(gus, downs):
    S = jax.ShapeDtypeStruct
    layers = len(gus)
    gate, down = S((layers, *gus[0].shape[1:]), BF16), S((layers, *downs[0].shape), BF16)
    return pl.pallas_call(
        functools.partial(finish_kernel, layers),
        out_shape=[gate, gate, down],
        in_specs=[pl.BlockSpec(memory_space=pltpu.VMEM)] * (2 * layers),
        out_specs=[pl.BlockSpec(memory_space=pl.ANY)] * 3,
        scratch_shapes=[pltpu.SemaphoreType.DMA((layers, 3))],
        compiler_params=pltpu.CompilerParams(vmem_limit_bytes=2**20),
        name="finish",
    )(*gus, *downs)


def solution(mesh):
    side = math.isqrt(mesh.shape["dp"])

    def step(x, dy, *arrays):
        weights, m, v = (arrays[i : i + 3] for i in (0, 3, 6))
        layers = weights[0].shape[0]

        a0, a0t, h1, a1, a1t, dyt = forward(x[0], dy[0], *weights)
        acts = (h1, a1, a1t, dy[0], dyt, a0, a0t)
        sums = backward(side, weights[0].shape[0], acts, weights, m[0].shape[1], m[2].shape[1])
        own_gu, own_d, moments = adam(sums, weights, m, v, side * side)
        return (*gather(side, own_gu, own_d), *moments)

    whole, block = P(None, None, None), P(None, "dp", None)
    return jax.shard_map(
        step,
        mesh=mesh,
        in_specs=(P(("rep", "dp"), None, None),) * 2 + (whole,) * 3 + (block,) * 6,
        out_specs=(P("rep", None, None),) * 3 + (P("rep", "dp", None),) * 6,
        check_vma=False,
    )
```

```python
import functools
import math

import jax
import jax.numpy as jnp
from jax import lax
from jax.experimental import pallas as pl
from jax.experimental.pallas import tpu as pltpu
from jax.sharding import PartitionSpec as P

MESH = pl.DeviceIdType.MESH
F32, BF16 = jnp.float32, jnp.bfloat16
QUARTERS = 4
PIECES = 2
CHUNKS = 4
TILE = 512
STEPS_AT = (((2, 1),), ((3, 3), (1, 0)), ((2, 2),))


NT = (((1,), (1,)), ((), ()))

def dot(a, b): return jnp.dot(a, b, preferred_element_type=F32)
def dot_nt(a, b): return lax.dot_general(a, b, NT, preferred_element_type=F32)

def normed(h):
    wide = h.astype(F32)
    scale = lax.rsqrt(jnp.mean(wide**2, -1, keepdims=True) + 1e-6)
    return (wide * scale).astype(BF16)

def forward_kernel(x, dy, wg, wu, wd, a0, a0t, h1, a1, a1t, dyt):
    a = normed(x[...])
    a0[...] = a
    a0t[...] = a.T
    dyt[...] = dy[...].T
    gate = dot(a, wg[...])
    up = dot(a, wu[...])
    p = (jax.nn.silu(gate) * up).astype(BF16)
    h = x[...] + dot(p, wd[...]).astype(BF16)
    h1[...] = h
    b = normed(h)
    a1[...] = b
    a1t[...] = b.T

def forward(x, dy, wg, wu, wd, T=256):
    n, d = x.shape
    f = wg.shape[2]
    tile = pl.BlockSpec((T, d), lambda i: (i, 0))
    tilet = pl.BlockSpec((d, T), lambda i: (0, i))
    const = lambda s: pl.BlockSpec((None, *s), lambda i: (0, 0, 0), pipeline_mode=pl.Buffered(1))
    S = jax.ShapeDtypeStruct
    return pl.pallas_call(
        forward_kernel, grid=(n // T,),
        in_specs=[tile, tile, const((d, f)), const((d, f)), const((f, d))],
        out_specs=[tile, tilet, tile, tile, tilet, tilet],
        out_shape=[S((n, d), BF16), S((d, n), BF16), S((n, d), BF16), S((n, d), BF16), S((d, n), BF16), S((d, n), BF16)],
        compiler_params=pltpu.CompilerParams(vmem_limit_bytes=60 * 2**20),
        name="fwd",
    )(x, dy, wg, wu, wd)


def tile_step(a, dy, wg, wu, wd):
    gate = dot(a, wg)
    up = dot(a, wu)
    dp = dot_nt(dy, wd).astype(BF16).astype(F32)
    s = jax.nn.sigmoid(gate)
    act = gate * s
    p = (act * up).astype(BF16)
    du = (dp * act).astype(BF16)
    dg = (dp * up * (s + act * (1.0 - s))).astype(BF16)
    return p, dg, du

def norm_back(h, da, dy):
    wide = h.astype(F32)
    d = h.shape[-1]
    scale = lax.rsqrt(jnp.mean(wide**2, -1, keepdims=True) + 1e-6)
    along = jnp.sum(da * wide, -1, keepdims=True)
    back = da * scale - wide * (along * (scale * scale * scale) * (1.0 / d))
    return (dy.astype(F32) + back.astype(BF16).astype(F32)).astype(BF16)

def adamw(w, m, v, g):
    m = 0.9 * m + 0.1 * g
    v = 0.95 * v + 0.05 * g * g
    step = m * lax.rsqrt(v + 1e-8) + 0.1 * w
    return (w - 0.02 * step).astype(BF16), m, v


class Torus:
    def __init__(self, side):
        self.side, self.n = side, side * side
        self.me = lax.axis_index("dp")
        self.row, self.col = lax.div(self.me, side), lax.rem(self.me, side)

    def greet(self):
        barrier = pltpu.get_barrier_semaphore()

        def one(k, _):
            pl.semaphore_signal(barrier, inc=1, device_id={"dp": lax.rem(self.me + k, self.n)}, device_id_type=MESH)
            return _

        lax.fori_loop(1, self.n, one, 0)
        pl.semaphore_wait(barrier, self.n - 1)

    def place(self, q):
        return (self.row, self.col) if q < 2 else (self.col, self.row)

    def wrap(self, k):
        return lax.rem(k + 2 * self.side, self.side)

    def device(self, q, u, v):
        u, v = self.wrap(u), self.wrap(v)
        return {"dp": u * self.side + v if q < 2 else v * self.side + u}

    def sign(self, q):
        return 1 if q % 2 == 0 else -1


def backward_kernel(side, layers, *refs):
    h1, a1, a1t, dy, dyt, a0, a0t, wg, wu, wd, sum_gu, sum_d, squares = refs[:13]
    (A, AT, DY, DYT, wgb, wub, wdb, ps, gs, us, das, loc_gu, loc_d, in1_gu, in1_d, in2_gu, in2_d, norms, tile) = refs[13:32]
    act_sem, w_sem, send_gu, recv_gu, send_d, recv_d, send_p, recv_p, norm_send, norm_recv = refs[32:]
    here = Torus(side)
    place, wrap, device, sign = here.place, here.wrap, here.device, here.sign
    n, d = A.shape
    F = wgb.shape[2]
    T = TILE
    width = F // QUARTERS
    steps = side - 1
    last = layers - 1

    wide = loc_d.shape[4]

    def across(k, i):
        return lax.rem(lax.rem(k, CHUNKS) + side - i, side)

    def units(k, i):
        return pl.ds(pl.multiple_of((i * side + across(k, i)) * wide, 128), wide)

    def weights(k):
        l, slot = last - lax.div(k, CHUNKS), lax.rem(k, 2)
        copies = []
        for i in range(side):
            of, to = units(k, i), pl.ds(i * wide, wide)
            copies += [
                pltpu.make_async_copy(wg.at[l, :, of], wgb.at[slot, :, to], w_sem.at[slot, 0, i]),
                pltpu.make_async_copy(wu.at[l, :, of], wub.at[slot, :, to], w_sem.at[slot, 1, i]),
                pltpu.make_async_copy(wd.at[l, of], wdb.at[slot, to], w_sem.at[slot, 2, i]),
            ]
        return copies

    loads = [pltpu.make_async_copy(x, y, act_sem.at[k]) for k, (x, y) in enumerate(((a1, A), (dy, DY), (a1t, AT), (dyt, DYT)))]
    for one in (loads[0], loads[1], *weights(0), loads[2], loads[3]):
        one.start()
    here.greet()
    tile[...] = jnp.zeros_like(tile)
    das[...] = jnp.zeros_like(das)
    for one in loads[:2]:
        one.wait()

    def strip(q):
        return pl.ds(q * (d // QUARTERS), d // QUARTERS)

    def lanes(k, q):
        return units(k, q)

    def sems(gu, k, q, s):
        return (send_gu.at[k, q, s], recv_gu.at[k, q, s]) if gu else (send_d.at[k, q, s], recv_d.at[k, q, s])

    def first(k, q, s):
        mu, mv = place(q)
        g = sign(q)
        if s == 0:
            u = wrap(mu - g)
            src = loc_gu.at[:, u, :, :, lanes(k, q)] if q < 2 else loc_gu.at[:, :, u, :, lanes(k, q)]
        else:
            src = in1_gu.at[k, q, s - 1]
        a, b = sems(True, k, q, s)
        return pltpu.make_async_remote_copy(src, in1_gu.at[k, q, s], a, b, device_id=device(q, mu + g, mv), device_id_type=MESH)

    def piece(k, q, s):
        l = last - lax.div(k, CHUNKS)
        mu, mv = place(q)
        g = sign(q)
        u = wrap(mu - g * (s + 1))
        v = across(k, u)
        if s == 0:
            src = loc_d.at[l, u, v, strip(q)] if q < 2 else loc_d.at[l, v, u, strip(q)]
        else:
            src = in1_d.at[l, q, s - 1, v]
        return pltpu.make_async_remote_copy(
            src, in1_d.at[l, q, s, v], send_p.at[k, q, s], recv_p.at[k, q, s], device_id=device(q, mu + g, mv), device_id_type=MESH)

    def second(gu, k, q, s):
        mu, mv = place(q)
        v = wrap(mv + sign(q) * (s + 1))
        src, dst = (in1_gu.at[k, q, steps - 1, :, v], in2_gu.at[k, q, s]) if gu else (in1_d.at[k, q, steps - 1, v], in2_d.at[k, q, s])
        a, b = sems(gu, k, q, steps + s if gu else s)
        return pltpu.make_async_remote_copy(src, dst, a, b, device_id=device(q, mu, v), device_id_type=MESH)

    def add_first(k, q, s):
        u = wrap(place(q)[0] - sign(q) * (s + 2))

        def one(v, _):
            a, b = (u, v) if q < 2 else (v, u)
            mine = loc_gu[:, a, b, :, lanes(k, q)].astype(F32)
            in1_gu[k, q, s, :, v] = (in1_gu[k, q, s, :, v].astype(F32) + mine).astype(BF16)
            return _

        if s < steps - 1:
            lax.fori_loop(0, side, one, 0)
        else:
            lax.fori_loop(1, side, lambda v, _: one(wrap(place(q)[1] + v), _), 0)

    def add_piece(k, q, s):
        l = last - lax.div(k, CHUNKS)
        u = wrap(place(q)[0] - sign(q) * (s + 2))
        v = across(k, u)
        a, b = (u, v) if q < 2 else (v, u)

        def add():
            mine = loc_d[l, a, b, strip(q)].astype(F32)
            in1_d[l, q, s, v] = (in1_d[l, q, s, v].astype(F32) + mine).astype(BF16)

        if s < steps - 1:
            add()
        else:
            pl.when(v != place(q)[1])(add)

    def add_second(gu, k, q):
        mv = place(q)[1]
        if gu:
            total = loc_gu[:, here.row, here.col, :, lanes(k, q)].astype(F32) + in1_gu[k, q, steps - 1, :, mv].astype(F32)
        else:
            total = loc_d[k, here.row, here.col, strip(q)].astype(F32) + in1_d[k, q, steps - 1, mv].astype(F32)
        for s in range(steps):
            total += (in2_gu if gu else in2_d)[k, q, s].astype(F32)
        total = total.astype(BF16)
        total = total.astype(F32)
        if gu:
            sum_gu[:, last - lax.div(k, CHUNKS), :, lanes(k, q)] = total
        else:
            sum_d[k, strip(q)] = total
        square = total * total
        square = square.reshape(-1, 8, square.shape[-1]).sum(0)
        tile[...] += sum(square[:, i : i + 128] for i in range(0, square.shape[-1], 128))

    def begin(k):
        for q in range(QUARTERS):
            first(k, q, 0).start()
            piece(k, q, 0).start()

    def turn_down(l):
        for q in range(QUARTERS):
            for s in range(steps):
                second(False, l, q, s).start()

    def advance(gu, k, s):
        for q in range(QUARTERS):
            if s < steps:
                first(k, q, s).wait()
                add_first(k, q, s)
                if s + 1 < steps:
                    first(k, q, s + 1).start()
                else:
                    for i in range(steps):
                        second(True, k, q, i).start()
                piece(k, q, s).wait()
                add_piece(k, q, s)
                if s + 1 < steps:
                    piece(k, q, s + 1).start()
            else:
                for i in range(steps):
                    second(gu, k, q, i).wait()
                add_second(gu, k, q)

    def chunk(k, inner):
        slot = lax.rem(k, 2)
        for one in weights(k):
            one.wait()

        @pl.when(k + 1 < layers * CHUNKS)
        def _():
            for one in weights(k + 1):
                one.start()

        def ticks(point):
            for back, step in STEPS_AT[point]:
                if inner:
                    pl.when(k >= back)(lambda: advance(True, k - back, step))
                else:
                    advance(True, k - back, step)

        for t in range(n // T):
            ts = pl.ds(t * T, T)
            p, dg, du = tile_step(A[ts], DY[ts], wgb[slot], wub[slot], wdb[slot])
            ps[ts] = p
            gs[ts] = dg
            us[ts] = du
            if inner:
                das[ts] += dot_nt(dg, wgb[slot]) + dot_nt(du, wub[slot])
            if t % 2 == 1:
                ticks(t // 2)
        if inner:
            @pl.when(k == 0)
            def _():
                for one in loads[2:]:
                    one.wait()

        rows = loc_gu.shape[3]
        for which, of in ((0, gs), (1, us)):
            g = dot(AT[...], of[...]).astype(BF16)
            for i in range(side * side):
                for j in range(side):
                    loc_gu[which, i // side, i % side, :, units(k, j)] = g[i * rows : (i + 1) * rows, j * wide : (j + 1) * wide]
        l = last - lax.div(k, CHUNKS)
        g = dot(DYT[...], ps[...]).astype(BF16)
        for i in range(side):
            loc_d[l, i, across(k, i)] = g[:, i * wide : (i + 1) * wide]
        ticks(2)
        begin(k)

    lax.fori_loop(0, CHUNKS, lambda k, _: (chunk(k, True), _)[1], 0)

    again = [pltpu.make_async_copy(x, y, act_sem.at[k]) for k, (x, y) in enumerate(((h1, A), (a0, A), (a0t, AT)))]
    again[0].start()
    again[2].start()
    again[0].wait()

    def turn(t, _):
        ts = pl.ds(pl.multiple_of(t * 256, 256), 256)
        r = norm_back(A[ts], das[ts].astype(BF16).astype(F32), DY[ts])
        DY[ts] = r
        DYT[:, ts] = r.T
        return _

    lax.fori_loop(0, n // 256, turn, 0)
    again[1].start()
    again[1].wait()
    again[2].wait()

    def outer(k, _):
        chunk(k, False)

        pl.when(k == CHUNKS + 1)(lambda: turn_down(last))
        pl.when(k == CHUNKS + 2)(lambda: advance(False, last, steps))
        return _

    lax.fori_loop(CHUNKS, layers * CHUNKS, outer, 0)
    end = layers * CHUNKS - 1
    for s in range(steps + 1):
        for k, done in ((end - 2, 3), (end - 1, 1), (end, 0)):
            if done + s <= steps:
                advance(True, k, done + s)
        if s == steps - 1:
            turn_down(0)
    advance(False, 0, steps)

    norms[here.me] = tile[...]

    def share(k):
        return pltpu.make_async_remote_copy(
            tile, norms.at[here.me], norm_send.at[k], norm_recv.at[k],
            device_id={"dp": lax.rem(here.me + k, here.n)}, device_id_type=MESH)

    lax.fori_loop(1, here.n, lambda k, _: (share(k).start(), _)[1], 0)
    lax.fori_loop(1, here.n, lambda k, _: (share(k).wait(), _)[1], 0)
    squares[...] = jnp.sum(norms[...], axis=0)


def backward(side, layers, acts, weights, rows, deep):
    n, d = acts[0].shape
    f = weights[0].shape[2]
    F = f // CHUNKS
    width = F // QUARTERS
    assert CHUNKS == QUARTERS == side and width == deep
    steps = side - 1
    S, V = jax.ShapeDtypeStruct, pltpu.VMEM
    jobs = layers * CHUNKS
    vmem, hbm = pl.BlockSpec(memory_space=pltpu.VMEM), pl.BlockSpec(memory_space=pl.ANY)
    return pl.pallas_call(
        functools.partial(backward_kernel, side, layers),
        out_shape=[S((2, layers, rows, f), F32), S((layers, d, deep), F32), S((8, 128), F32)],
        in_specs=[hbm] * 10,
        out_specs=[vmem] * 3,
        scratch_shapes=[
            V((n, d), BF16), V((d, n), BF16), V((n, d), BF16), V((d, n), BF16),
            V((2, d, F), BF16), V((2, d, F), BF16), V((2, F, d), BF16),
            V((n, F), BF16), V((n, F), BF16), V((n, F), BF16), V((n, d), F32),
            V((2, side, side, rows, f), BF16),
            V((layers, side, side, d, deep), BF16),
            V((jobs, QUARTERS, steps, 2, side, rows, width), BF16),
            V((layers, QUARTERS, steps, side, d // QUARTERS, deep), BF16),
            V((jobs, QUARTERS, steps, 2, rows, width), BF16),
            V((layers, QUARTERS, steps, d // QUARTERS, deep), BF16),
            V((side * side, 8, 128), F32), V((8, 128), F32),
            pltpu.SemaphoreType.DMA((4,)),
            pltpu.SemaphoreType.DMA((2, 3, side)),
            pltpu.SemaphoreType.DMA((jobs, QUARTERS, 2 * steps)),
            pltpu.SemaphoreType.DMA((jobs, QUARTERS, 2 * steps)),
            pltpu.SemaphoreType.DMA((layers, QUARTERS, steps)),
            pltpu.SemaphoreType.DMA((layers, QUARTERS, steps)),
            pltpu.SemaphoreType.DMA((jobs, QUARTERS, steps)),
            pltpu.SemaphoreType.DMA((jobs, QUARTERS, steps)),
            pltpu.SemaphoreType.DMA((side * side,)),
            pltpu.SemaphoreType.DMA((side * side,)),
        ],
        compiler_params=pltpu.CompilerParams(collective_id=0, has_side_effects=True, vmem_limit_bytes=67043328),
        name="bwd",
    )(*acts, *weights)


def adam_kernel(count, me, gate, up, down, sum_gu, sum_d, squares, *refs):
    m, v, own, nm, nv = refs[:3], refs[3:6], refs[6:8], refs[8:11], refs[11:]
    total = jnp.sum(squares[...])
    factor = jnp.minimum(1.0, 0.5 * lax.rsqrt(jnp.full((1, 1), total, F32) / count + 1e-30))
    for k, w in enumerate((gate, up)):
        own[0][k], nm[k][...], nv[k][...] = adamw(w[...].astype(F32), m[k][...], v[k][...], sum_gu[k] * factor)
    own[1][...], nm[2][...], nv[2][...] = adamw(down[...].astype(F32), m[2][...], v[2][...], sum_d[...].T * factor)


def adam(sums, w, m, v, n):
    layers, rows, cols = m[0].shape
    deep, narrow = m[2].shape[1:]
    S = jax.ShapeDtypeStruct
    wide, tall = (None, rows, cols), (None, deep, narrow)
    mine = lambda s: pl.BlockSpec(s, lambda l, me: (l, me[0], 0))
    whole = lambda s: pl.BlockSpec(s, lambda l, me: (l, 0, 0))
    both = pl.BlockSpec((2, None, rows, cols), lambda l, me: (0, l, 0, 0))
    moments = [whole(wide), whole(wide), whole(tall)]
    outs = pl.pallas_call(
        functools.partial(adam_kernel, layers * n * (2 * rows * cols + deep * narrow)),
        grid_spec=pltpu.PrefetchScalarGridSpec(
            num_scalar_prefetch=1,
            grid=(layers,),
            in_specs=[mine(wide), mine(wide), mine(tall), both, whole((None, narrow, deep)), pl.BlockSpec((8, 128), lambda l, me: (0, 0)), *moments, *moments],
            out_specs=[both, whole(tall), *moments, *moments],
        ),
        out_shape=[S((2, layers, rows, cols), BF16), S((layers, deep, narrow), BF16), *(S(t.shape, F32) for t in (*m, *v))],
        compiler_params=pltpu.CompilerParams(vmem_limit_bytes=62 * 2**20),
        name="adam",
    )(lax.axis_index("dp").reshape(1), *w, *sums, *m, *v)
    return outs[0], outs[1], outs[2:]


def gather_kernel(side, layers, *refs):
    own_gu, own_d = refs[:2]
    new_gu, new_d = refs[2 : 2 + layers], refs[2 + layers : 2 + 2 * layers]
    send_gu, recv_gu, send_d, recv_d = refs[2 + 2 * layers :]
    here = Torus(side)
    place, wrap, device, sign, row, col = here.place, here.wrap, here.device, here.sign, here.row, here.col
    steps = side - 1
    cols = own_gu.shape[3]
    quarter = own_d.shape[1] // QUARTERS
    width = cols // PIECES // QUARTERS
    for l in range(layers):
        new_gu[l][:, row, col] = own_gu[:, l]
        for q in range(QUARTERS):
            new_d[l][row, col, q] = own_d[l, q * quarter : (q + 1) * quarter]
    here.greet()

    def lanes(h, q):
        return pl.ds(pl.multiple_of((h * QUARTERS + q) * width, 128), width)

    def sems(l, h, q, s):
        if h is None:
            return send_d.at[l, q, s], recv_d.at[l, q, s]
        return send_gu.at[l, h, q, s], recv_gu.at[l, h, q, s]

    def jobs(f):
        for l in reversed(range(layers)):
            lax.fori_loop(0, PIECES, lambda h, _: (f(l, h), _)[1], 0)
            f(l, None)

    def gather(l, h, q, s):
        mu, mv = place(q)
        g = sign(q)
        gu, down = new_gu[l], new_d[l]
        if s < steps:
            v = wrap(mv - g * s)
            a, b = (mu, v) if q < 2 else (v, mu)
            src = dst = down.at[a, b, q] if h is None else gu.at[:, a, b, :, lanes(h, q)]
            if s == 0:
                src = own_d.at[l, pl.ds(q * quarter, quarter)] if h is None else own_gu.at[:, l, :, lanes(h, q)]
            to = device(q, mu, mv + g)
        else:
            u = wrap(mu - g * (s - steps))
            if h is None:
                dst = down.at[u, :, q] if q < 2 else down.at[:, u, q]
            else:
                dst = gu.at[:, u, :, :, lanes(h, q)] if q < 2 else gu.at[:, :, u, :, lanes(h, q)]
            src = dst
            to = device(q, mu + g, mv)
        a, b = sems(l, h, q, s)
        return pltpu.make_async_remote_copy(src, dst, a, b, device_id=to, device_id_type=MESH)

    def begin(l, h):
        for q in range(QUARTERS):
            gather(l, h, q, 0).start()

    jobs(begin)
    for s in range(2 * steps):
        def advance(l, h, s=s):
            for q in range(QUARTERS):
                gather(l, h, q, s).wait()
                if s + 1 < 2 * steps:
                    gather(l, h, q, s + 1).start()

        jobs(advance)


def gather(side, own_gu, own_d):
    layers, rows, cols = own_gu.shape[1:]
    deep, narrow = own_d.shape[1:]
    n = side * side
    steps = side - 1
    vmem = pl.BlockSpec(memory_space=pltpu.VMEM)
    S = jax.ShapeDtypeStruct
    outs = pl.pallas_call(
        functools.partial(gather_kernel, side, layers),
        out_shape=[S((2, side, side, rows, cols), BF16)] * layers + [S((side, side, QUARTERS, deep // QUARTERS, narrow), BF16)] * layers,
        in_specs=[vmem] * 2,
        out_specs=[vmem] * (2 * layers),
        scratch_shapes=[
            pltpu.SemaphoreType.DMA((layers, PIECES, QUARTERS, 2 * steps)),
            pltpu.SemaphoreType.DMA((layers, PIECES, QUARTERS, 2 * steps)),
            pltpu.SemaphoreType.DMA((layers, QUARTERS, 2 * steps)),
            pltpu.SemaphoreType.DMA((layers, QUARTERS, 2 * steps)),
        ],
        compiler_params=pltpu.CompilerParams(collective_id=1, has_side_effects=True, vmem_limit_bytes=4 * 2**20),
        name="gather",
    )(own_gu, own_d)
    gus, downs = outs[:layers], outs[layers:]
    return finish([t.reshape(2, n * rows, cols) for t in gus], [t.reshape(n * deep, narrow) for t in downs])


def finish_kernel(layers, *refs):
    gus, downs, (gate, up, down, sem) = refs[:layers], refs[layers : 2 * layers], refs[2 * layers :]
    copies = []
    for l in range(layers):
        for k, (x, y) in enumerate(((gus[l].at[0], gate), (gus[l].at[1], up), (downs[l], down))):
            copies.append(pltpu.make_async_copy(x, y.at[l], sem.at[l, k]))
    for one in copies:
        one.start()
    for one in copies:
        one.wait()


def finish(gus, downs):
    S = jax.ShapeDtypeStruct
    layers = len(gus)
    gate, down = S((layers, *gus[0].shape[1:]), BF16), S((layers, *downs[0].shape), BF16)
    return pl.pallas_call(
        functools.partial(finish_kernel, layers),
        out_shape=[gate, gate, down],
        in_specs=[pl.BlockSpec(memory_space=pltpu.VMEM)] * (2 * layers),
        out_specs=[pl.BlockSpec(memory_space=pl.ANY)] * 3,
        scratch_shapes=[pltpu.SemaphoreType.DMA((layers, 3))],
        compiler_params=pltpu.CompilerParams(vmem_limit_bytes=2**20),
        name="finish",
    )(*gus, *downs)


def solution(mesh):
    side = math.isqrt(mesh.shape["dp"])

    def step(x, dy, *arrays):
        weights, m, v = (arrays[i : i + 3] for i in (0, 3, 6))
        layers = weights[0].shape[0]

        a0, a0t, h1, a1, a1t, dyt = forward(x[0], dy[0], *weights)
        acts = (h1, a1, a1t, dy[0], dyt, a0, a0t)
        sums = backward(side, weights[0].shape[0], acts, weights, m[0].shape[1], m[2].shape[1])
        own_gu, own_d, moments = adam(sums, weights, m, v, side * side)
        return (*gather(side, own_gu, own_d), *moments)

    whole, block = P(None, None, None), P(None, "dp", None)
    return jax.shard_map(
        step,
        mesh=mesh,
        in_specs=(P(("rep", "dp"), None, None),) * 2 + (whole,) * 3 + (block,) * 6,
        out_specs=(P("rep", None, None),) * 3 + (P("rep", "dp", None),) * 6,
        check_vma=False,
    )
```
